8 devices in a mesh: batch: 1 (over z), cy: 2 (over y), cx: 4 (over x, core).
Axes of the slice: x: 2, y: 2, z: 1, core: 2. Of those that a mesh axis runs over, the one named last changes fastest.
Arguments:
- q: bfloat16 [1536, 64, 128], P(('batch', 'cy', 'cx'))
- k: bfloat16 [1536, 8, 128], P(('batch', 'cy', 'cx'))
- v: bfloat16 [1536, 8, 128], P(('batch', 'cy', 'cx'))
Outputs:
- output: bfloat16 [1536, 64, 128], P(('batch', 'cy', 'cx'))
All inputs are finite; a program needn't handle non-finite values.
Results may differ from the reference program's by a relative error of at most 0.00212845.
Values are sent between devices in bfloat16 or wider.
A program may use at most 1 GiB of HBM per device.

```python
import jax
import jax.numpy as jnp
from jax import lax

HEADS = 64
KV_HEADS = 8
HEAD_DIM = 128
TOK = 192
NDEV = 8
QB = 32

SEQ = NDEV * TOK
CH = TOK // 2
GQ = HEADS // KV_HEADS


def piece_and_position():
    i = jnp.arange(SEQ, dtype=jnp.int32)
    r = i // TOK
    w = i % TOK
    piece = jnp.where(w < CH, r, 2 * NDEV - 1 - r)
    return piece, piece * CH + w % CH


def setup_inputs(seed: int = 0, part: int = 0) -> dict:
    key = jax.random.fold_in(jax.random.key(seed), part)
    kq, kk, kv, ko = jax.random.split(key, 4)
    piece, pos = piece_and_position()
    q = jax.random.normal(kq, (SEQ, HEADS, HEAD_DIM), jnp.float32)
    k = jax.random.normal(kk, (SEQ, KV_HEADS, HEAD_DIM), jnp.float32)
    offs = jax.random.normal(ko, (2 * NDEV, KV_HEADS, HEAD_DIM), jnp.float32)
    v = offs[piece] + 0.5 * jax.random.normal(kv, (SEQ, KV_HEADS, HEAD_DIM), jnp.float32)
    return {'q': q.astype(jnp.bfloat16), 'k': k.astype(jnp.bfloat16), 'v': v.astype(jnp.bfloat16)}


def reference(q, k, v):
    piece, pos = piece_and_position()
    scale = HEAD_DIM ** -0.5
    kf = k.astype(jnp.float32)
    vf = v.astype(jnp.float32)
    qb = q.reshape(SEQ // QB, QB, KV_HEADS, GQ, HEAD_DIM)
    pb = pos.reshape(SEQ // QB, QB)

    def one(xs):
        qi, pi = xs
        s = jnp.einsum('qkgd,skd->kgqs', qi.astype(jnp.float32), kf) * scale
        s = jnp.where(pos[None, :] <= pi[:, None], s, -jnp.inf)
        mx = jnp.max(s, axis=-1, keepdims=True)
        p = jnp.exp(s - mx)
        l = jnp.sum(p, axis=-1)
        o = jnp.einsum('kgqs,skd->qkgd', p.astype(jnp.bfloat16).astype(jnp.float32), vf)
        o = o / jnp.transpose(l, (2, 0, 1))[..., None]
        return o.reshape(QB, HEADS, HEAD_DIM).astype(jnp.bfloat16)

    return lax.map(one, (qb, pb)).reshape(SEQ, HEADS, HEAD_DIM)
```

```python
import functools
import math

import jax
import jax.numpy as jnp
from jax import lax
from jax.experimental import pallas as pl
from jax.experimental.pallas import tpu as pltpu
from jax.sharding import PartitionSpec as P

MESH = pl.DeviceIdType.MESH
AHEAD = 2
QT = 32


def kernel(q_hbm, k_hbm, v_hbm, o_ref, q_s, raw, f32s, kv, vt, s_s, p_s,
           load_sem, send_sem, recv_sem, *, nchip, groups, piece, scale):
    G, CH = groups, piece
    GQ, D = q_s.shape[2], q_s.shape[3]
    NP = kv.shape[1]
    cb = lax.axis_index('batch')
    cy = lax.axis_index('cy')
    cx = lax.axis_index('cx')
    ox = lax.rem(cx + 2, 4)
    sx = cx + 1 - 2 * lax.rem(cx, 2)
    osx = ox + 1 - 2 * lax.rem(ox, 2)
    oy = 1 - cy
    x_dev = (cb, cy, ox)
    y_dev = (cb, oy, cx)
    s_dev = (cb, cy, sx)
    me = cy * 4 + cx
    rx, ry, rd = cy * 4 + ox, oy * 4 + cx, oy * 4 + ox
    sib = (cy * 4 + sx, cy * 4 + osx, oy * 4 + sx, oy * 4 + osx)
    hi = lambda r: NP - 1 - r

    kcopy = pltpu.make_async_copy(k_hbm, raw.at[0], load_sem.at[0])
    vcopy = pltpu.make_async_copy(v_hbm, raw.at[1], load_sem.at[1])
    kcopy.start()
    vcopy.start()

    barrier = pltpu.get_barrier_semaphore()
    for dev in (x_dev, y_dev, s_dev):
        pl.semaphore_signal(barrier, inc=1, device_id=dev, device_id_type=MESH)

    qcopies = [pltpu.make_async_copy(q_hbm.at[:, g], q_s.at[g], load_sem.at[2 + g]) for g in range(G)]
    for c in qcopies:
        c.start()

    for which, copy in ((0, kcopy), (1, vcopy)):
        copy.wait()
        f32s[...] = raw[which].astype(jnp.float32).reshape(2 * CH * G, D)
        for g in range(G):
            rows = f32s[pl.ds(g, 2 * CH, stride=G), :].astype(jnp.bfloat16)
            kv[g, me, which] = rows[:CH]
            kv[g, hi(me), which] = rows[CH:]

    pl.semaphore_wait(barrier, 3)

    def remote(g, p, slot, dev):
        return pltpu.make_async_remote_copy(
            src_ref=kv.at[g, p], dst_ref=kv.at[g, p], send_sem=send_sem.at[g, slot],
            recv_sem=recv_sem.at[g, p], device_id=dev, device_id_type=MESH)

    def recv(g, p):
        remote(g, p, 0, x_dev).wait_recv()

    own = ((me, 0, x_dev), (me, 1, y_dev), (hi(me), 2, x_dev), (hi(me), 3, y_dev),
           (me, 4, s_dev), (hi(me), 5, s_dev))
    cross = ((rx, 6, y_dev), (hi(ry), 7, x_dev))
    side = ((rx, 8, s_dev), (hi(rx), 9, s_dev), (ry, 10, s_dev), (hi(ry), 11, s_dev))
    last = ((rd, 12, s_dev), (hi(rd), 13, s_dev))

    def start(g, sends):
        for p, slot, dev in sends:
            remote(g, p, slot, dev).start()

    def forward(g):
        for p in (rx, hi(rx), ry, hi(ry)):
            recv(g, p)
        start(g, cross + side)

    def diagonal(g):
        recv(g, rd)
        recv(g, hi(rd))
        start(g, last)

    def rest(g):
        for r in sib:
            recv(g, r)
            recv(g, hi(r))

    c2 = scale * math.log2(math.e)
    row = lax.broadcasted_iota(jnp.int32, (2 * CH, QT * GQ), 0)
    tok = lax.broadcasted_iota(jnp.int32, (2 * CH, QT * GQ), 1) // GQ
    odd = lax.rem(cx, 2)

    def attend(g, chip):
        tiles = []
        for half in (1, 0):
            nch = (nchip * 2 - chip) if half else (chip + 1)
            off = CH * ((1 - odd) if half else odd)
            for t in range(CH // QT):
                tiles.append((half, nch, off, t))
        n_all = 2 * CH * (nchip * 2 - chip)
        vt[:, :n_all] = kv[g, 0:n_all // CH, 1].reshape(n_all, D).T

        def scores(tile, buf):
            half, nch, off, t = tile
            qv = q_s[g, half * CH + t * QT:half * CH + (t + 1) * QT].reshape(QT * GQ, D)
            m8 = None
            for j in range(nch):
                kb = kv[g, 2 * j:2 * j + 2, 0].reshape(2 * CH, D)
                s = lax.dot_general(kb, qv, (((1,), (1,)), ((), ())), preferred_element_type=jnp.float32)
                if j == nch - 1:
                    s = jnp.where(row - tok <= off + t * QT, s, -jnp.inf)
                s_s[buf, j * 2 * CH:(j + 1) * 2 * CH] = s
                mj = jnp.max(s.reshape(2 * CH // 8, 8, QT * GQ), axis=0)
                m8 = mj if m8 is None else jnp.maximum(m8, mj)
            return jnp.max(m8, axis=0, keepdims=True)

        def finish(tile, buf, m):
            half, nch, off, t = tile
            l8 = None
            for j in range(nch):
                sl = slice(j * 2 * CH, (j + 1) * 2 * CH)
                p = jnp.exp2((s_s[buf, sl] - m) * c2)
                lj = jnp.sum(p.reshape(2 * CH // 8, 8, QT * GQ), axis=0)
                l8 = lj if l8 is None else l8 + lj
                p_s[buf, sl] = p.astype(jnp.bfloat16)
            n = nch * 2 * CH
            l = jnp.sum(l8, axis=0, keepdims=True)
            acc = lax.dot_general(vt[:, :n], p_s[buf, :n], (((1,), (0,)), ((), ())),
                                  preferred_element_type=jnp.float32)
            out = (acc * (1.0 / l)).T.astype(jnp.bfloat16)
            o_ref[half * CH + t * QT:half * CH + (t + 1) * QT, g] = out.reshape(QT, GQ, D)

        m = scores(tiles[0], 0)
        for idx, tile in enumerate(tiles):
            if idx + 1 < len(tiles):
                m_next = scores(tiles[idx + 1], (idx + 1) % 2)
            finish(tile, idx % 2, m)
            m = m_next

    for g in range(AHEAD):
        start(g, own)
    for c in qcopies:
        c.wait()

    chip_of = me // 2

    def step(i, carry):
        @pl.when(i < G)
        def _():
            forward(i)

        @pl.when(i < G - AHEAD)
        def _():
            start(i + AHEAD, own)

        @pl.when(i > 0)
        def _():
            g = i - 1
            diagonal(g)
            rest(g)
            for chip in range(nchip):
                @pl.when(chip_of == chip)
                def _(chip=chip):
                    attend(g, chip)
        return carry

    lax.fori_loop(0, G + 1, step, 0)

    def drain(g, carry):
        for p, slot, dev in own + cross + side + last:
            remote(g, p, slot, dev).wait_send()
        return carry

    lax.fori_loop(0, G, drain, 0)


def solution(mesh):
    spec = P(('batch', 'cy', 'cx'), None, None)

    def local(q, k, v):
        t, h, d = q.shape
        kvh = k.shape[1]
        gq = h // kvh
        ch = t // 2
        ndev = mesh.shape['cy'] * mesh.shape['cx']
        npieces = 2 * ndev
        n = ndev * t
        body = functools.partial(kernel, nchip=ndev // 2, groups=kvh, piece=ch, scale=d ** -0.5)
        any_spec = pl.BlockSpec(memory_space=pltpu.HBM)
        out = pl.pallas_call(
            body,
            out_shape=jax.ShapeDtypeStruct((t, kvh, gq, d), jnp.bfloat16),
            in_specs=[any_spec] * 3,
            out_specs=pl.BlockSpec(memory_space=pltpu.VMEM),
            scratch_shapes=[
                pltpu.VMEM((kvh, t, gq, d), jnp.bfloat16),
                pltpu.VMEM((2, t, kvh, d), jnp.bfloat16),
                pltpu.VMEM((t * kvh, d), jnp.float32),
                pltpu.VMEM((kvh, npieces, 2, ch, d), jnp.bfloat16),
                pltpu.VMEM((d, n), jnp.bfloat16),
                pltpu.VMEM((2, n, QT * gq), jnp.float32),
                pltpu.VMEM((2, n, QT * gq), jnp.bfloat16),
                pltpu.SemaphoreType.DMA((2 + kvh,)),
                pltpu.SemaphoreType.DMA((kvh, 14)),
                pltpu.SemaphoreType.DMA((kvh, npieces)),
            ],
            compiler_params=pltpu.CompilerParams(
                collective_id=0, has_side_effects=True, vmem_limit_bytes=40 * 2**20),
            name='ring_attention',
        )(*[pltpu.with_memory_space_constraint(x, pltpu.HBM) for x in (q.reshape(t, kvh, gq, d), k, v)])
        return out.reshape(t, h, d)

    return jax.shard_map(local, mesh=mesh, in_specs=(spec, spec, spec), out_specs=spec, check_vma=False)
```

```python
import functools
import math

import jax
import jax.numpy as jnp
from jax import lax
from jax.experimental import pallas as pl
from jax.experimental.pallas import tpu as pltpu
from jax.sharding import PartitionSpec as P

MESH = pl.DeviceIdType.MESH
AHEAD = 2
QT = 32
NT = 3
NEG = -jnp.inf


def chunks_of(chip):
    far = 3 - chip
    early_low = [(0, j) for j in range(chip + 1) if j != far]
    late_low = [(0, far)] if far <= chip else []
    early_high = early_low + [(0, j) for j in range(chip + 1, 4) if j != far]
    early_high += [(1, j) for j in range(3, chip - 1, -1) if j != far]
    late_high = [(0, far)] + ([(1, far)] if far >= chip else [])
    return early_high, early_low, late_high, late_low


def kernel(q_hbm, k_hbm, v_hbm, o_ref, q_s, raw, f32s, kv, vte, vtl, *rest,
           scale):
    s_s, p_s, m_s, al_s, be_s, l_s = (rest[3 * i:3 * i + 3] for i in range(6))
    mk, lk, acck, load_sem, send_sem, xy_sem, dg_sem, se_sem, sl_sem = rest[18:]
    G, T, GQ, D = q_s.shape
    CH = T // 2
    C2 = 2 * CH
    W = QT * GQ
    cb = lax.axis_index('batch')
    cy = lax.axis_index('cy')
    cx = lax.axis_index('cx')
    ox = lax.rem(cx + 2, 4)
    sx = cx + 1 - 2 * lax.rem(cx, 2)
    oy = 1 - cy
    x_dev = (cb, cy, ox)
    y_dev = (cb, oy, cx)
    s_dev = (cb, cy, sx)
    me = cy * 4 + cx
    rx, ry, rd = cy * 4 + ox, oy * 4 + cx, oy * 4 + ox
    odd = lax.rem(cx, 2)
    chip_of = me // 2

    kcopy = pltpu.make_async_copy(k_hbm, raw.at[0], load_sem.at[0])
    vcopy = pltpu.make_async_copy(v_hbm, raw.at[1], load_sem.at[1])
    kcopy.start()
    vcopy.start()

    barrier = pltpu.get_barrier_semaphore()
    for dev in (x_dev, y_dev, s_dev):
        pl.semaphore_signal(barrier, inc=1, device_id=dev, device_id_type=MESH)

    for g in range(G):
        pltpu.make_async_copy(q_hbm.at[:, g], q_s.at[g], load_sem.at[2]).start()

    def take(g):
        for which in (0, 1):
            rows = f32s[which, pl.ds(g, T, stride=G), :].astype(jnp.bfloat16)
            kv[g, me, 0, which] = rows[:CH]
            kv[g, me, 1, which] = rows[CH:]

    for which, copy in ((0, kcopy), (1, vcopy)):
        copy.wait()
        f32s[which] = raw[which].astype(jnp.float32).reshape(T * G, D)
    for g in range(AHEAD):
        take(g)

    pl.semaphore_wait(barrier, 3)

    def block(g, r):
        return kv.at[g, r]

    def send(g, ref, recv_sem, dev):
        pltpu.make_async_remote_copy(
            src_ref=ref, dst_ref=ref, send_sem=send_sem.at[g], recv_sem=recv_sem.at[g],
            device_id=dev, device_id_type=MESH).start()

    def arrived(g, count, recv_sem):
        ref = kv.at[g, 0:count]
        pltpu.make_async_remote_copy(
            src_ref=ref, dst_ref=ref, send_sem=send_sem.at[g], recv_sem=recv_sem.at[g],
            device_id=x_dev, device_id_type=MESH).wait_recv()

    def start_own(g):
        send(g, kv.at[g, me], xy_sem, x_dev)
        send(g, kv.at[g, me], xy_sem, y_dev)
        send(g, kv.at[g, me], se_sem, s_dev)

    def forward(g):
        arrived(g, 2, xy_sem)
        send(g, kv.at[g, rx, 0], dg_sem, y_dev)
        send(g, kv.at[g, ry, 1], dg_sem, x_dev)
        send(g, kv.at[g, rx], se_sem, s_dev)
        send(g, kv.at[g, ry], se_sem, s_dev)

    def diagonal(g):
        arrived(g, 1, dg_sem)
        send(g, kv.at[g, rd], sl_sem, s_dev)

    for g in range(AHEAD):
        start_own(g)
    for g in range(AHEAD, G):
        take(g)
    pltpu.make_async_copy(q_s, q_s, load_sem.at[2]).wait()

    c2 = scale * math.log2(math.e)
    sub = lax.broadcasted_iota(jnp.int32, (8, W), 0)
    base = sub - lax.broadcasted_iota(jnp.int32, (8, W), 1) // GQ

    def keys(g, chunk_list, which):
        parts = [kv[g, 2 * j:2 * j + 2, half, which].reshape(C2, D) for half, j in chunk_list]
        return parts[0] if len(parts) == 1 else jnp.concatenate(parts, axis=0)

    def pipeline(chip):
        lists = chunks_of(chip)
        names = ('eh', 'el', 'lh', 'll')
        rows = {}
        at = 0
        for name, lst in zip(names, lists):
            rows[name] = (at, C2 * len(lst))
            at += C2 * len(lst)
        lst = dict(zip(names, lists))
        halves = (1, 0)

        def transposed(g, slot, names):
            for name, ref in names:
                n = rows[name][1]
                ref[slot, :, :n] = keys(g, lst[name], 1).T

        def split(u):
            return lax.div(u + NT, NT) - 1, lax.rem(u + NT, NT)

        def score(g, t, half, name, slot, masked):
            at, n = rows[name]
            qv = q_s[g, pl.ds(half * CH + t * QT, QT)].reshape(W, D)
            s = lax.dot_general(keys(g, lst[name], 0), qv, (((1,), (1,)), ((), ())),
                                preferred_element_type=jnp.float32)
            edge = n - C2 if masked else n
            top = None
            if edge:
                s_s[slot][at:at + edge] = s[:edge]
                for i in range(edge // 8):
                    si = s[8 * i:8 * i + 8]
                    top = si if top is None else jnp.maximum(top, si)
            if masked:
                thr = t * QT + CH * (odd if half == 0 else -odd)
                for i in range(C2 // 8):
                    first = 8 * i if (half == 0 or i < CH // 8) else 8 * i - C2
                    si = jnp.where(base <= thr - first, s[edge + 8 * i:edge + 8 * i + 8], NEG)
                    s_s[slot][at + edge + 8 * i:at + edge + 8 * i + 8] = si
                    top = si if top is None else jnp.maximum(top, si)
            return jnp.max(top, axis=0, keepdims=True)

        def stage_a(u, slot, early=True, late=True):
            g, t = split(u)
            gl = jnp.where(g == 0, G, g - 1)
            ql = jnp.maximum(g - 1, 0)
            for half in halves:
                e, l = ('eh', 'lh') if half else ('el', 'll')
                if late and lst[l]:
                    old = mk[half, t]
                    m = jnp.maximum(score_late(gl, ql, t, half, l, slot), old)
                    m_s[slot][2 + half] = m
                    al_s[slot][half] = jnp.exp2((old - m) * c2)
                if early:
                    m = score(g, t, half, e, slot, True)
                    m_s[slot][half] = m
                    mk[half, t] = m

        def score_late(gl, ql, t, half, name, slot):
            at, n = rows[name]
            qv = q_s[ql, pl.ds(half * CH + t * QT, QT)].reshape(W, D)
            s = lax.dot_general(keys(gl, lst[name], 0), qv, (((1,), (1,)), ((), ())),
                                preferred_element_type=jnp.float32)
            s_s[slot][at:at + n] = s
            top = s[:8]
            for i in range(1, n // 8):
                top = jnp.maximum(top, s[8 * i:8 * i + 8])
            return jnp.max(top, axis=0, keepdims=True)

        def weights(name, slot, m):
            at, n = rows[name]
            total = None
            for j in range(n // C2):
                sl = slice(at + j * C2, at + (j + 1) * C2)
                p = jnp.exp2((s_s[slot][sl] - m) * c2)
                for i in range(C2 // 8):
                    pi = p[8 * i:8 * i + 8]
                    total = pi if total is None else total + pi
                p_s[slot][sl] = p.astype(jnp.bfloat16)
            return jnp.sum(total, axis=0, keepdims=True)

        def stage_b(u, slot, early=True, late=True):
            g, t = split(u)
            for half in halves:
                e, l = ('eh', 'lh') if half else ('el', 'll')
                if late and lst[l]:
                    total = weights(l, slot, m_s[slot][2 + half])
                    l_s[slot][2 + half] = lk[half, t] * al_s[slot][half] + total
                    be_s[slot][half] = al_s[slot][half]
                if early:
                    total = weights(e, slot, m_s[slot][half])
                    l_s[slot][half] = total
                    lk[half, t] = total

        def values(name, ref, par, slot):
            at, n = rows[name]
            return lax.dot_general(ref[par, :, :n], p_s[slot][at:at + n], (((1,), (0,)), ((), ())),
                                   preferred_element_type=jnp.float32)

        def put(g, t, half, acc, total):
            out = (acc * (1.0 / total)).astype(jnp.bfloat16).T
            o_ref[pl.ds(half * CH + t * QT, QT), g] = out.reshape(QT, GQ, D)

        def stage_c(u, slot, early=True, late=True):
            g, t = split(u)
            ge = jnp.maximum(g, 0)
            gl = jnp.maximum(g - 1, 0)
            for half in halves:
                e, l = ('eh', 'lh') if half else ('el', 'll')
                if late and lst[l]:
                    acc = acck[half, t] * be_s[slot][half] + values(l, vtl, lax.rem(gl, 2), slot)
                    put(gl, t, half, acc, l_s[slot][2 + half])
                if early:
                    acc = values(e, vte, lax.rem(ge, 2), slot)
                    if lst[l]:
                        acck[half, t] = acc
                    else:
                        put(ge, t, half, acc, l_s[slot][half])

        def service(g):
            @pl.when(g < G - 1)
            def _():
                forward(g + 1)

            @pl.when(g < G - 1 - AHEAD)
            def _():
                start_own(g + 1 + AHEAD)

            @pl.when(g < G - 1)
            def _():
                diagonal(g)

            arrived(g, 3, se_sem)

            @pl.when(g > 0)
            def _():
                arrived(g - 1, 1, sl_sem)
                transposed(g - 1, lax.rem(g - 1, 2), (('lh', vtl),))
            transposed(g, lax.rem(g, 2), (('eh', vte),))

        def body(pair, carry):
            for odd_i in (0, 1):
                i = 2 * pair + odd_i

                @pl.when(lax.rem(i, NT) == 0)
                def _(i=i):
                    service(lax.div(i, NT))

                stage_b(i - 1, 1 - odd_i)
                stage_a(i, odd_i)
                stage_c(i - 2, odd_i)
            return carry

        n = NT * G
        lax.fori_loop(0, n // 2, body, 0)
        stage_c(n - 2, n % 2)
        stage_b(n - 1, 1 - n % 2)
        stage_c(n - 1, 1 - n % 2)

        diagonal(G - 1)
        arrived(G - 1, 1, sl_sem)
        transposed(G - 1, (G - 1) % 2, (('lh', vtl),))
        tail(stage_a, stage_b, stage_c, n)

    def tail(stage_a, stage_b, stage_c, n):
        for t in range(NT):
            stage_a(n + t, t, early=False)
        for t in range(NT):
            stage_b(n + t, t, early=False)
        for t in range(NT):
            stage_c(n + t, t, early=False)

    forward(0)
    start_own(AHEAD)
    for chip in range(4):
        @pl.when(chip_of == chip)
        def _(chip=chip):
            pipeline(chip)

    def drain(g, carry):
        ref = kv.at[g, 0:7]
        pltpu.make_async_remote_copy(
            src_ref=ref, dst_ref=ref, send_sem=send_sem.at[g], recv_sem=xy_sem.at[g],
            device_id=x_dev, device_id_type=MESH).wait_send()
        return carry

    lax.fori_loop(0, G, drain, 0)


def solution(mesh):
    spec = P(('batch', 'cy', 'cx'), None, None)

    def local(q, k, v):
        t, h, d = q.shape
        kvh = k.shape[1]
        gq = h // kvh
        ch = t // 2
        ndev = mesh.shape['cy'] * mesh.shape['cx']
        w = QT * gq
        rows = 9 * 2 * ch
        any_spec = pl.BlockSpec(memory_space=pltpu.HBM)
        operands = [pltpu.with_memory_space_constraint(x, pltpu.HBM) for x in (q.reshape(t, kvh, gq, d), k, v)]
        out = pl.pallas_call(
            functools.partial(kernel, scale=d ** -0.5),
            out_shape=jax.ShapeDtypeStruct((t, kvh, gq, d), jnp.bfloat16),
            in_specs=[any_spec] * 3,
            out_specs=pl.BlockSpec(memory_space=pltpu.VMEM),
            scratch_shapes=[
                pltpu.VMEM((kvh, t, gq, d), jnp.bfloat16),
                pltpu.VMEM((2, t, kvh, d), jnp.bfloat16),
                pltpu.VMEM((2, t * kvh, d), jnp.float32),
                pltpu.VMEM((kvh + 1, ndev, 2, 2, ch, d), jnp.bfloat16),
                pltpu.VMEM((2, d, 12 * ch), jnp.bfloat16),
                pltpu.VMEM((2, d, 4 * ch), jnp.bfloat16),
                *[pltpu.VMEM((rows, w), jnp.float32)] * 3,
                *[pltpu.VMEM((rows, w), jnp.bfloat16)] * 3,
                *[pltpu.VMEM((4, 1, w), jnp.float32)] * 3,
                *[pltpu.VMEM((2, 1, w), jnp.float32)] * 6,
                *[pltpu.VMEM((4, 1, w), jnp.float32)] * 3,
                pltpu.VMEM((2, NT, 1, w), jnp.float32),
                pltpu.VMEM((2, NT, 1, w), jnp.float32),
                pltpu.VMEM((2, NT, d, w), jnp.float32),
                pltpu.SemaphoreType.DMA((3,)),
                *[pltpu.SemaphoreType.DMA((kvh,))] * 5,
            ],
            compiler_params=pltpu.CompilerParams(
                collective_id=0, has_side_effects=True, vmem_limit_bytes=40 * 2**20),
            name='ring_attention',
        )(*operands)
        return out.reshape(t, h, d)

    return jax.shard_map(local, mesh=mesh, in_specs=(spec, spec, spec), out_specs=spec, check_vma=False)
```

```python
import functools
import math

import jax
import jax.numpy as jnp
from jax import lax
from jax.experimental import pallas as pl
from jax.experimental.pallas import tpu as pltpu
from jax.sharding import PartitionSpec as P

MESH = pl.DeviceIdType.MESH
AHEAD = 2
QT = 32
NT = 3
NEG = -jnp.inf


def chunks_of(chip):
    far = 3 - chip
    early_low = [(0, j) for j in range(chip + 1) if j != far]
    late_low = [(0, far)] if far <= chip else []
    early_high = early_low + [(0, j) for j in range(chip + 1, 4) if j != far]
    early_high += [(1, j) for j in range(3, chip - 1, -1) if j != far]
    late_high = [(0, far)] + ([(1, far)] if far >= chip else [])
    return early_high, early_low, late_high, late_low


def kernel(q_hbm, k_hbm, v_hbm, o_ref, q_last, kv_last, mk, lk, acck, q_s, raw, f32s, kv, vte, vtl, *rest,
           scale):
    s_s, p_s, m_s, al_s, be_s, l_s = (rest[3 * i:3 * i + 3] for i in range(6))
    load_sem, send_sem, xy_sem, dg_sem, se_sem, sl_sem = rest[18:]
    G, T, GQ, D = q_s.shape
    CH = T // 2
    C2 = 2 * CH
    W = QT * GQ
    cb = lax.axis_index('batch')
    cy = lax.axis_index('cy')
    cx = lax.axis_index('cx')
    ox = lax.rem(cx + 2, 4)
    sx = cx + 1 - 2 * lax.rem(cx, 2)
    oy = 1 - cy
    x_dev = (cb, cy, ox)
    y_dev = (cb, oy, cx)
    s_dev = (cb, cy, sx)
    me = cy * 4 + cx
    rx, ry, rd = cy * 4 + ox, oy * 4 + cx, oy * 4 + ox
    odd = lax.rem(cx, 2)
    chip_of = me // 2

    kcopy = pltpu.make_async_copy(k_hbm, raw.at[0], load_sem.at[0])
    vcopy = pltpu.make_async_copy(v_hbm, raw.at[1], load_sem.at[1])
    kcopy.start()
    vcopy.start()

    barrier = pltpu.get_barrier_semaphore()
    for dev in (x_dev, y_dev, s_dev):
        pl.semaphore_signal(barrier, inc=1, device_id=dev, device_id_type=MESH)

    for g in range(G):
        pltpu.make_async_copy(q_hbm.at[:, g], q_s.at[g], load_sem.at[2]).start()

    def take(g):
        for which in (0, 1):
            rows = f32s[which, pl.ds(g, T, stride=G), :].astype(jnp.bfloat16)
            kv[g, 2 * me, which] = rows[:CH]
            kv[g, 2 * me + 1, which] = rows[CH:]

    for which, copy in ((0, kcopy), (1, vcopy)):
        copy.wait()
        f32s[which] = raw[which].astype(jnp.float32).reshape(T * G, D)
    for g in range(AHEAD):
        take(g)

    pl.semaphore_wait(barrier, 3)

    def piece(g, r, full):
        return kv.at[g, pl.ds(2 * r, 2)] if full else kv.at[g, 2 * r]

    def send(g, ref, recv_sem, dev):
        pltpu.make_async_remote_copy(
            src_ref=ref, dst_ref=ref, send_sem=send_sem.at[g], recv_sem=recv_sem.at[g],
            device_id=dev, device_id_type=MESH).start()

    def arrived(g, count, recv_sem):
        ref = kv.at[g, 0:count]
        pltpu.make_async_remote_copy(
            src_ref=ref, dst_ref=ref, send_sem=send_sem.at[g], recv_sem=recv_sem.at[g],
            device_id=x_dev, device_id_type=MESH).wait_recv()

    c2 = scale * math.log2(math.e)
    sub = lax.broadcasted_iota(jnp.int32, (8, W), 0)
    base = sub - lax.broadcasted_iota(jnp.int32, (8, W), 1) // GQ

    def keys(g, chunk_list, which):
        parts = [kv[g, 4 * j + half + 2 * core, which] for half, j in chunk_list for core in (0, 1)]
        return jnp.concatenate(parts, axis=0)

    def pipeline(chip):
        xc, yc, far = chip ^ 1, chip ^ 2, chip ^ 3
        own_x, own_y = True, True
        got_x, got_y, got_far = True, True, True
        cross_high = True
        n_xy = 2 + got_x + got_y
        n_far = 1 + got_far
        n_sent = (2 + own_x + own_y) + 2 + (1 + cross_high) + (2 + got_x + got_y) + n_far

        def start_own(g):
            send(g, piece(g, me, own_x), xy_sem, x_dev)
            send(g, piece(g, me, own_y), xy_sem, y_dev)
            send(g, piece(g, me, True), se_sem, s_dev)

        def forward(g):
            arrived(g, n_xy, xy_sem)
            send(g, kv.at[g, 2 * rx], dg_sem, y_dev)
            if cross_high:
                send(g, kv.at[g, 2 * ry + 1], dg_sem, x_dev)
            send(g, piece(g, rx, got_x), se_sem, s_dev)
            send(g, piece(g, ry, got_y), se_sem, s_dev)

        def diagonal(g):
            arrived(g, n_far, dg_sem)
            send(g, piece(g, rd, got_far), sl_sem, s_dev)

        for g in range(AHEAD):
            start_own(g)
        for g in range(AHEAD, G):
            take(g)
        pltpu.make_async_copy(q_s, q_s, load_sem.at[2]).wait()
        q_last[...] = q_s[G - 1]

        lists = chunks_of(chip)
        names = ('eh', 'el', 'lh', 'll')
        rows = {}
        at = 0
        for name, lst in zip(names, lists):
            rows[name] = (at, C2 * len(lst))
            at += C2 * len(lst)
        lst = dict(zip(names, lists))
        halves = (1, 0)

        def transposed(g, slot, names):
            for name, ref in names:
                n = rows[name][1]
                ref[slot, :, :n] = keys(g, lst[name], 1).T

        def split(u):
            return lax.div(u + NT, NT) - 1, lax.rem(u + NT, NT)

        def score(g, t, half, name, slot, masked):
            at, n = rows[name]
            qv = q_s[g, pl.ds(half * CH + t * QT, QT)].reshape(W, D)
            s = lax.dot_general(keys(g, lst[name], 0), qv, (((1,), (1,)), ((), ())),
                                preferred_element_type=jnp.float32)
            edge = n - C2 if masked else n
            top = None
            if edge:
                s_s[slot][at:at + edge] = s[:edge]
                for i in range(edge // 8):
                    si = s[8 * i:8 * i + 8]
                    top = si if top is None else jnp.maximum(top, si)
            if masked:
                thr = t * QT + CH * (odd if half == 0 else -odd)
                for i in range(C2 // 8):
                    first = 8 * i if (half == 0 or i < CH // 8) else 8 * i - C2
                    si = jnp.where(base <= thr - first, s[edge + 8 * i:edge + 8 * i + 8], NEG)
                    s_s[slot][at + edge + 8 * i:at + edge + 8 * i + 8] = si
                    top = si if top is None else jnp.maximum(top, si)
            return jnp.max(top, axis=0, keepdims=True)

        def stage_a(u, slot, early=True, late=True):
            g, t = split(u)
            gl = jnp.where(g == 0, G, g - 1)
            ql = jnp.maximum(g - 1, 0)
            for half in halves:
                e, l = ('eh', 'lh') if half else ('el', 'll')
                if late and lst[l]:
                    old = mk[half, t]
                    m = jnp.maximum(score_late(gl, ql, t, half, l, slot), old)
                    m_s[slot][2 + half] = m
                    al_s[slot][half] = jnp.exp2((old - m) * c2)
                if early:
                    m = score(g, t, half, e, slot, True)
                    m_s[slot][half] = m
                    mk[half, t] = m

        def score_late(gl, ql, t, half, name, slot):
            at, n = rows[name]
            qv = q_s[ql, pl.ds(half * CH + t * QT, QT)].reshape(W, D)
            s = lax.dot_general(keys(gl, lst[name], 0), qv, (((1,), (1,)), ((), ())),
                                preferred_element_type=jnp.float32)
            s_s[slot][at:at + n] = s
            top = s[:8]
            for i in range(1, n // 8):
                top = jnp.maximum(top, s[8 * i:8 * i + 8])
            return jnp.max(top, axis=0, keepdims=True)

        def weights(name, slot, m):
            at, n = rows[name]
            total = None
            for j in range(n // C2):
                sl = slice(at + j * C2, at + (j + 1) * C2)
                p = jnp.exp2((s_s[slot][sl] - m) * c2)
                for i in range(C2 // 8):
                    pi = p[8 * i:8 * i + 8]
                    total = pi if total is None else total + pi
                p_s[slot][sl] = p.astype(jnp.bfloat16)
            return jnp.sum(total, axis=0, keepdims=True)

        def stage_b(u, slot, early=True, late=True):
            g, t = split(u)
            for half in halves:
                e, l = ('eh', 'lh') if half else ('el', 'll')
                if late and lst[l]:
                    total = weights(l, slot, m_s[slot][2 + half])
                    l_s[slot][2 + half] = lk[half, t] * al_s[slot][half] + total
                    be_s[slot][half] = al_s[slot][half]
                if early:
                    total = weights(e, slot, m_s[slot][half])
                    l_s[slot][half] = total
                    lk[half, t] = total

        def values(name, ref, par, slot):
            at, n = rows[name]
            return lax.dot_general(ref[par, :, :n], p_s[slot][at:at + n], (((1,), (0,)), ((), ())),
                                   preferred_element_type=jnp.float32)

        def put(g, t, half, acc, total):
            out = (acc * (1.0 / total)).astype(jnp.bfloat16).T
            o_ref[pl.ds(half * CH + t * QT, QT), g] = out.reshape(QT, GQ, D)

        def stage_c(u, slot, early=True, late=True):
            g, t = split(u)
            ge = jnp.maximum(g, 0)
            gl = jnp.maximum(g - 1, 0)
            for half in halves:
                e, l = ('eh', 'lh') if half else ('el', 'll')
                if late and lst[l]:
                    acc = acck[half, t] * be_s[slot][half] + values(l, vtl, lax.rem(gl, 2), slot)
                    put(gl, t, half, acc, l_s[slot][2 + half])
                if early:
                    acc = values(e, vte, lax.rem(ge, 2), slot)
                    if lst[l]:
                        acck[half, t] = acc
                    else:
                        put(ge, t, half, acc, l_s[slot][half])

        def service(g):
            @pl.when(g < G - 1)
            def _():
                forward(g + 1)

            arrived(g, 2 + n_xy, se_sem)

            @pl.when(g > 0)
            def _():
                arrived(g - 1, n_far, sl_sem)
                transposed(g - 1, lax.rem(g - 1, 2), (('lh', vtl),))
            transposed(g, lax.rem(g, 2), (('eh', vte),))

        n = NT * G
        forward(0)
        start_own(AHEAD)

        def body(pair, carry):
            for odd_i in (0, 1):
                i = 2 * pair + odd_i

                @pl.when(lax.rem(i, NT) == 0)
                def _(i=i):
                    service(lax.div(i, NT))

                @pl.when(jnp.logical_and(lax.rem(i, NT) == 1, i < n - NT - NT * AHEAD))
                def _(i=i):
                    start_own(lax.div(i, NT) + 1 + AHEAD)

                @pl.when(jnp.logical_and(lax.rem(i, NT) == 1, i < n - NT))
                def _(i=i):
                    diagonal(lax.div(i, NT))

                stage_a(i, odd_i)
                stage_b(i - 1, 1 - odd_i)
                stage_c(i - 1, 1 - odd_i)
            return carry

        lax.fori_loop(0, n // 2, body, 0)
        stage_b(n - 1, 1 - n % 2)
        stage_c(n - 1, 1 - n % 2)

        diagonal(G - 1)
        arrived(G - 1, n_far, sl_sem)
        for i, (half, j) in enumerate(lst['lh']):
            for core in (0, 1):
                kv_last[2 * i + core] = kv[G - 1, 4 * j + half + 2 * core]

        def drain(g, carry):
            ref = kv.at[g, 0:n_sent]
            pltpu.make_async_remote_copy(
                src_ref=ref, dst_ref=ref, send_sem=send_sem.at[g], recv_sem=xy_sem.at[g],
                device_id=x_dev, device_id_type=MESH).wait_send()
            return carry

        lax.fori_loop(0, G, drain, 0)

    def tail(stage_a, stage_b, stage_c, n):
        for t in range(NT):
            stage_a(n + t, t, early=False)
        for t in range(NT):
            stage_b(n + t, t, early=False)
        for t in range(NT):
            stage_c(n + t, t, early=False)

    for chip in range(4):
        @pl.when(chip_of == chip)
        def _(chip=chip):
            pipeline(chip)


def last_kernel(o_part, q_last, kv_last, mk, lk, acck, o_hbm, out_s, s_s, p_s, sem, *, scale):
    T, G, GQ, D = o_part.shape
    CH = T // 2
    W = QT * GQ
    chip_of = lax.axis_index('cy') * 2 + lax.axis_index('cx') // 2
    step = T // 4
    copies = [pltpu.make_async_copy(o_part.at[pl.ds(i * step, step), pl.ds(0, G - 1)],
                                    o_hbm.at[pl.ds(i * step, step), pl.ds(0, G - 1)], sem.at[i]) for i in range(4)]
    for c in copies:
        c.start()
    c2 = scale * math.log2(math.e)

    def merge(chip):
        late_high, late_low = chunks_of(chip)[2:]
        tiles = [(1, t, len(late_high)) for t in range(NT)]
        tiles += [(0, t, len(late_low)) for t in range(NT) if late_low]
        ends = []
        if not late_low:
            ends.append(pltpu.make_async_copy(o_part.at[pl.ds(0, CH), G - 1], o_hbm.at[pl.ds(0, CH), G - 1], sem.at[G]))
            ends[0].start()
        n_pieces = 2 * len(late_high)
        keys = kv_last[0:n_pieces, 0].reshape(n_pieces * CH, D)
        vals = kv_last[0:n_pieces, 1].reshape(n_pieces * CH, D).T
        slabs = lambda x: [x[8 * i:8 * i + 8] for i in range(x.shape[0] // 8)]
        tops, sums, at = [], [], 0
        for half, t, count in tiles:
            n = 2 * CH * count
            rows = slice(half * CH + t * QT, half * CH + (t + 1) * QT)
            s = lax.dot_general(keys[:n], q_last[rows].reshape(W, D), (((1,), (1,)), ((), ())),
                                preferred_element_type=jnp.float32)
            s_s[at:at + n] = s
            top = functools.reduce(jnp.maximum, slabs(s))
            tops.append(jnp.maximum(jnp.max(top, axis=0, keepdims=True), mk[half, t]))
            at += n
        at = 0
        for (half, t, count), m in zip(tiles, tops):
            n = 2 * CH * count
            total = None
            for j in range(count):
                sl = slice(at + j * 2 * CH, at + (j + 1) * 2 * CH)
                p = jnp.exp2((s_s[sl] - m) * c2)
                part = functools.reduce(jnp.add, slabs(p))
                total = part if total is None else total + part
                p_s[sl] = p.astype(jnp.bfloat16)
            sums.append(jnp.sum(total, axis=0, keepdims=True))
            at += n
        at = 0
        for (half, t, count), m, total in zip(tiles, tops, sums):
            n = 2 * CH * count
            rows = slice(half * CH + t * QT, half * CH + (t + 1) * QT)
            alpha = jnp.exp2((mk[half, t] - m) * c2)
            inv = 1.0 / (lk[half, t] * alpha + total)
            acc = acck[half, t] * (alpha * inv) + lax.dot_general(
                vals[:, :n], p_s[at:at + n], (((1,), (0,)), ((), ())), preferred_element_type=jnp.float32) * inv
            out_s[rows] = acc.astype(jnp.bfloat16).T.reshape(QT, GQ, D)
            at += n
        for half in ((1, 0) if late_low else (1,)):
            ends.append(pltpu.make_async_copy(
                out_s.at[pl.ds(half * CH, CH)], o_hbm.at[pl.ds(half * CH, CH), G - 1], sem.at[G + 1 + half]))
            ends[-1].start()
        for c in ends:
            c.wait()

    for chip in range(4):
        @pl.when(chip_of == chip)
        def _(chip=chip):
            merge(chip)

    for c in copies:
        c.wait()


def solution(mesh):
    spec = P(('batch', 'cy', 'cx'), None, None)

    def local(q, k, v):
        t, h, d = q.shape
        kvh = k.shape[1]
        gq = h // kvh
        ch = t // 2
        ndev = mesh.shape['cy'] * mesh.shape['cx']
        w = QT * gq
        rows = 9 * 2 * ch
        any_spec = pl.BlockSpec(memory_space=pltpu.HBM)
        operands = [pltpu.with_memory_space_constraint(x, pltpu.HBM) for x in (q.reshape(t, kvh, gq, d), k, v)]
        states = [
            jax.ShapeDtypeStruct((t, kvh, gq, d), jnp.bfloat16),
            jax.ShapeDtypeStruct((t, gq, d), jnp.bfloat16),
            jax.ShapeDtypeStruct((4, 2, ch, d), jnp.bfloat16),
            jax.ShapeDtypeStruct((2, NT, 1, w), jnp.float32),
            jax.ShapeDtypeStruct((2, NT, 1, w), jnp.float32),
            jax.ShapeDtypeStruct((2, NT, d, w), jnp.float32),
        ]
        vmem = pl.BlockSpec(memory_space=pltpu.VMEM)
        states = pl.pallas_call(
            functools.partial(kernel, scale=d ** -0.5),
            out_shape=states,
            in_specs=[any_spec] * 3,
            out_specs=[vmem] * 6,
            scratch_shapes=[
                pltpu.VMEM((kvh, t, gq, d), jnp.bfloat16),
                pltpu.VMEM((2, t, kvh, d), jnp.bfloat16),
                pltpu.VMEM((2, t * kvh, d), jnp.float32),
                pltpu.VMEM((kvh + 1, 2 * ndev, 2, ch, d), jnp.bfloat16),
                pltpu.VMEM((2, d, 12 * ch), jnp.bfloat16),
                pltpu.VMEM((2, d, 4 * ch), jnp.bfloat16),
                *[pltpu.VMEM((rows, w), jnp.float32)] * 3,
                *[pltpu.VMEM((rows, w), jnp.bfloat16)] * 3,
                *[pltpu.VMEM((4, 1, w), jnp.float32)] * 3,
                *[pltpu.VMEM((2, 1, w), jnp.float32)] * 6,
                *[pltpu.VMEM((4, 1, w), jnp.float32)] * 3,
                pltpu.SemaphoreType.DMA((3,)),
                *[pltpu.SemaphoreType.DMA((kvh,))] * 5,
            ],
            compiler_params=pltpu.CompilerParams(
                collective_id=0, has_side_effects=True, vmem_limit_bytes=40 * 2**20),
            name='ring_attention',
        )(*operands)
        out = pl.pallas_call(
            functools.partial(last_kernel, scale=d ** -0.5),
            out_shape=jax.ShapeDtypeStruct((t, kvh, gq, d), jnp.bfloat16),
            in_specs=[vmem] * 6,
            out_specs=any_spec,
            scratch_shapes=[
                pltpu.VMEM((t, gq, d), jnp.bfloat16),
                pltpu.VMEM((12 * ch, w), jnp.float32),
                pltpu.VMEM((12 * ch, w), jnp.bfloat16),
                pltpu.SemaphoreType.DMA((kvh + 3,)),
            ],
            compiler_params=pltpu.CompilerParams(vmem_limit_bytes=16 * 2**20),
            name='write_result',
        )(*states)
        return out.reshape(t, h, d)

    return jax.shard_map(local, mesh=mesh, in_specs=(spec, spec, spec), out_specs=spec, check_vma=False)
```

```python
import functools
import math

import jax
import jax.numpy as jnp
from jax import lax
from jax.experimental import pallas as pl
from jax.experimental.pallas import tpu as pltpu
from jax.sharding import PartitionSpec as P

MESH = pl.DeviceIdType.MESH
AHEAD = 3
QT = 32
NT = 3
NEG = -jnp.inf


def chunks_of(chip):
    far = 3 - chip
    early_low = [(0, j) for j in range(chip + 1) if j != far]
    late_low = [(0, far)] if far <= chip else []
    early_high = early_low + [(0, j) for j in range(chip + 1, 4) if j != far]
    early_high += [(1, j) for j in range(3, chip - 1, -1) if j != far]
    late_high = [(0, far)] + ([(1, far)] if far >= chip else [])
    return early_high, early_low, late_high, late_low


def kernel(q_hbm, k_hbm, v_hbm, o_ref, q_last, kv_last, mk, lk, acck, q_s, raw, f32s, kv, vte, vtl, *rest,
           scale):
    s_s, p_s, m_s, al_s, be_s, l_s = (rest[3 * i:3 * i + 3] for i in range(6))
    load_sem, send_sem, xy_sem, dg_sem, se_sem, sl_sem = rest[18:]
    G, T, GQ, D = q_s.shape
    CH = T // 2
    C2 = 2 * CH
    W = QT * GQ
    cb = lax.axis_index('batch')
    cy = lax.axis_index('cy')
    cx = lax.axis_index('cx')
    ox = lax.rem(cx + 2, 4)
    sx = cx + 1 - 2 * lax.rem(cx, 2)
    oy = 1 - cy
    x_dev = (cb, cy, ox)
    y_dev = (cb, oy, cx)
    s_dev = (cb, cy, sx)
    me = cy * 4 + cx
    rx, ry, rd = cy * 4 + ox, oy * 4 + cx, oy * 4 + ox
    odd = lax.rem(cx, 2)
    chip_of = me // 2

    kcopy = pltpu.make_async_copy(k_hbm, raw.at[0], load_sem.at[0])
    vcopy = pltpu.make_async_copy(v_hbm, raw.at[1], load_sem.at[1])
    kcopy.start()
    vcopy.start()

    barrier = pltpu.get_barrier_semaphore()
    for dev in (x_dev, y_dev, s_dev):
        pl.semaphore_signal(barrier, inc=1, device_id=dev, device_id_type=MESH)

    for g in range(G):
        pltpu.make_async_copy(q_hbm.at[:, g], q_s.at[g], load_sem.at[2]).start()

    def take(g):
        for which in (0, 1):
            rows = f32s[which, pl.ds(g, T, stride=G), :].astype(jnp.bfloat16)
            kv[g, 2 * me, which] = rows[:CH]
            kv[g, 2 * me + 1, which] = rows[CH:]

    for which, copy in ((0, kcopy), (1, vcopy)):
        copy.wait()
        f32s[which] = raw[which].astype(jnp.float32).reshape(T * G, D)
    for g in range(AHEAD):
        take(g)

    pl.semaphore_wait(barrier, 3)

    def piece(g, r, full):
        return kv.at[g, pl.ds(2 * r, 2)] if full else kv.at[g, 2 * r]

    def send(g, ref, recv_sem, dev):
        pltpu.make_async_remote_copy(
            src_ref=ref, dst_ref=ref, send_sem=send_sem.at[g], recv_sem=recv_sem.at[g],
            device_id=dev, device_id_type=MESH).start()

    def arrived(g, count, recv_sem):
        ref = kv.at[g, 0:count]
        pltpu.make_async_remote_copy(
            src_ref=ref, dst_ref=ref, send_sem=send_sem.at[g], recv_sem=recv_sem.at[g],
            device_id=x_dev, device_id_type=MESH).wait_recv()

    c2 = scale * math.log2(math.e)
    sub = lax.broadcasted_iota(jnp.int32, (8, W), 0)
    base = sub - lax.broadcasted_iota(jnp.int32, (8, W), 1) // GQ

    def keys(g, chunk_list, which):
        parts = [kv[g, 4 * j + half + 2 * core, which] for half, j in chunk_list for core in (0, 1)]
        return jnp.concatenate(parts, axis=0)

    def pipeline(chip):
        xc, yc, far = chip ^ 1, chip ^ 2, chip ^ 3
        own_x, own_y = True, True
        got_x, got_y, got_far = True, True, True
        cross_high = True
        n_xy = 2 + got_x + got_y
        n_far = 1 + got_far
        n_sent = (2 + own_x + own_y) + 2 + (1 + cross_high) + (2 + got_x + got_y) + n_far

        def start_own(g):
            send(g, piece(g, me, own_x), xy_sem, x_dev)
            send(g, piece(g, me, own_y), xy_sem, y_dev)
            send(g, piece(g, me, True), se_sem, s_dev)

        def forward(g):
            arrived(g, n_xy, xy_sem)
            send(g, kv.at[g, 2 * rx], dg_sem, y_dev)
            if cross_high:
                send(g, kv.at[g, 2 * ry + 1], dg_sem, x_dev)
            send(g, piece(g, rx, got_x), se_sem, s_dev)
            send(g, piece(g, ry, got_y), se_sem, s_dev)

        def diagonal(g):
            arrived(g, n_far, dg_sem)
            send(g, piece(g, rd, got_far), sl_sem, s_dev)

        for g in range(AHEAD):
            start_own(g)
        for g in range(AHEAD, G):
            take(g)
        pltpu.make_async_copy(q_s, q_s, load_sem.at[2]).wait()
        q_last[...] = q_s[G - 1]

        lists = chunks_of(chip)
        names = ('eh', 'el', 'lh', 'll')
        rows = {}
        at = 0
        for name, lst in zip(names, lists):
            rows[name] = (at, C2 * len(lst))
            at += C2 * len(lst)
        lst = dict(zip(names, lists))
        halves = (1, 0)

        def transposed(g, slot, names):
            for name, ref in names:
                n = rows[name][1]
                ref[slot, :, :n] = keys(g, lst[name], 1).T

        def split(u):
            return lax.div(u + NT, NT) - 1, lax.rem(u + NT, NT)

        def score(g, t, half, name, slot, masked):
            at, n = rows[name]
            qv = q_s[g, pl.ds(half * CH + t * QT, QT)].reshape(W, D)
            s = lax.dot_general(keys(g, lst[name], 0), qv, (((1,), (1,)), ((), ())),
                                preferred_element_type=jnp.float32)
            edge = n - C2 if masked else n
            top = None
            if edge:
                s_s[slot][at:at + edge] = s[:edge]
                for i in range(edge // 8):
                    si = s[8 * i:8 * i + 8]
                    top = si if top is None else jnp.maximum(top, si)
            if masked:
                thr = t * QT + CH * (odd if half == 0 else -odd)
                for i in range(C2 // 8):
                    first = 8 * i if (half == 0 or i < CH // 8) else 8 * i - C2
                    si = jnp.where(base <= thr - first, s[edge + 8 * i:edge + 8 * i + 8], NEG)
                    s_s[slot][at + edge + 8 * i:at + edge + 8 * i + 8] = si
                    top = si if top is None else jnp.maximum(top, si)
            return jnp.max(top, axis=0, keepdims=True)

        def stage_a(u, slot, early=True, late=True):
            g, t = split(u)
            par = lax.rem(g + 2, 2)
            gl = jnp.where(g < 2, G, g - 2)
            ql = jnp.maximum(g - 2, 0)
            for half in halves:
                e, l = ('eh', 'lh') if half else ('el', 'll')
                if late and lst[l]:
                    old = mk[par, half, t]
                    m = jnp.maximum(score_late(gl, ql, t, half, l, slot), old)
                    m_s[slot][2 + half] = m
                    al_s[slot][half] = jnp.exp2((old - m) * c2)
                if early:
                    m = score(g, t, half, e, slot, True)
                    m_s[slot][half] = m
                    mk[par, half, t] = m

        def score_late(gl, ql, t, half, name, slot):
            at, n = rows[name]
            qv = q_s[ql, pl.ds(half * CH + t * QT, QT)].reshape(W, D)
            s = lax.dot_general(keys(gl, lst[name], 0), qv, (((1,), (1,)), ((), ())),
                                preferred_element_type=jnp.float32)
            s_s[slot][at:at + n] = s
            top = s[:8]
            for i in range(1, n // 8):
                top = jnp.maximum(top, s[8 * i:8 * i + 8])
            return jnp.max(top, axis=0, keepdims=True)

        def weights(name, slot, m):
            at, n = rows[name]
            total = None
            for j in range(n // C2):
                sl = slice(at + j * C2, at + (j + 1) * C2)
                p = jnp.exp2((s_s[slot][sl] - m) * c2)
                for i in range(C2 // 8):
                    pi = p[8 * i:8 * i + 8]
                    total = pi if total is None else total + pi
                p_s[slot][sl] = p.astype(jnp.bfloat16)
            return jnp.sum(total, axis=0, keepdims=True)

        def stage_b(u, slot, early=True, late=True):
            g, t = split(u)
            par = lax.rem(g + 2, 2)
            for half in halves:
                e, l = ('eh', 'lh') if half else ('el', 'll')
                if late and lst[l]:
                    total = weights(l, slot, m_s[slot][2 + half])
                    l_s[slot][2 + half] = lk[par, half, t] * al_s[slot][half] + total
                    be_s[slot][half] = al_s[slot][half]
                if early:
                    total = weights(e, slot, m_s[slot][half])
                    l_s[slot][half] = total
                    lk[par, half, t] = total

        def values(name, ref, par, slot):
            at, n = rows[name]
            return lax.dot_general(ref[par, :, :n], p_s[slot][at:at + n], (((1,), (0,)), ((), ())),
                                   preferred_element_type=jnp.float32)

        def put(g, t, half, acc, total):
            out = (acc * (1.0 / total)).astype(jnp.bfloat16).T
            o_ref[pl.ds(half * CH + t * QT, QT), g] = out.reshape(QT, GQ, D)

        def stage_c(u, slot, early=True, late=True):
            g, t = split(u)
            par = lax.rem(g + 2, 2)
            ge = jnp.maximum(g, 0)
            gl = jnp.maximum(g - 2, 0)
            for half in halves:
                e, l = ('eh', 'lh') if half else ('el', 'll')
                if late and lst[l]:
                    acc = acck[par, half, t] * be_s[slot][half] + values(l, vtl, lax.rem(gl, 2), slot)
                    put(gl, t, half, acc, l_s[slot][2 + half])
                if early:
                    acc = values(e, vte, lax.rem(ge, 2), slot)
                    if lst[l]:
                        acck[par, half, t] = acc
                    else:
                        put(ge, t, half, acc, l_s[slot][half])

        def service(g):
            arrived(g, 2 + n_xy, se_sem)

            @pl.when(g > 1)
            def _():
                arrived(g - 2, n_far, sl_sem)
                transposed(g - 2, lax.rem(g, 2), (('lh', vtl),))
            transposed(g, lax.rem(g, 2), (('eh', vte),))

        n = NT * G
        forward(0)
        start_own(AHEAD)

        def body(pair, carry):
            for odd_i in (0, 1):
                i = 2 * pair + odd_i

                @pl.when(lax.rem(i, NT) == 0)
                def _(i=i):
                    service(lax.div(i, NT))

                @pl.when(jnp.logical_and(lax.rem(i, NT) == 1, i < n - NT))
                def _(i=i):
                    forward(lax.div(i, NT) + 1)

                @pl.when(jnp.logical_and(lax.rem(i, NT) == 1, i < n - NT - NT * AHEAD))
                def _(i=i):
                    start_own(lax.div(i, NT) + 1 + AHEAD)

                @pl.when(jnp.logical_and(lax.rem(i, NT) == 2, i >= NT))
                def _(i=i):
                    diagonal(lax.div(i, NT) - 1)

                stage_a(i, odd_i)
                stage_b(i - 1, 1 - odd_i)
                stage_c(i - 1, 1 - odd_i)
            return carry

        lax.fori_loop(0, n // 2, body, 0)
        stage_b(n - 1, 1 - n % 2)
        stage_c(n - 1, 1 - n % 2)

        diagonal(G - 1)
        arrived(G - 2, n_far, sl_sem)
        transposed(G - 2, G % 2, (('lh', vtl),))
        for t in range(NT):
            stage_a(n + t, t, early=False)
        for t in range(NT):
            stage_b(n + t, t, early=False)
        for t in range(NT):
            stage_c(n + t, t, early=False)
        arrived(G - 1, n_far, sl_sem)
        for i, (half, j) in enumerate(lst['lh']):
            for core in (0, 1):
                kv_last[2 * i + core] = kv[G - 1, 4 * j + half + 2 * core]

        def drain(g, carry):
            ref = kv.at[g, 0:n_sent]
            pltpu.make_async_remote_copy(
                src_ref=ref, dst_ref=ref, send_sem=send_sem.at[g], recv_sem=xy_sem.at[g],
                device_id=x_dev, device_id_type=MESH).wait_send()
            return carry

        lax.fori_loop(0, G, drain, 0)

    for chip in range(4):
        @pl.when(chip_of == chip)
        def _(chip=chip):
            pipeline(chip)


def last_kernel(o_part, q_last, kv_last, mk, lk, acck, o_hbm, out_s, s_s, p_s, sem, *, scale):
    T, G, GQ, D = o_part.shape
    CH = T // 2
    W = QT * GQ
    chip_of = lax.axis_index('cy') * 2 + lax.axis_index('cx') // 2
    step = T // 4
    copies = [pltpu.make_async_copy(o_part.at[pl.ds(i * step, step), pl.ds(0, G - 1)],
                                    o_hbm.at[pl.ds(i * step, step), pl.ds(0, G - 1)], sem.at[i]) for i in range(4)]
    for c in copies:
        c.start()
    c2 = scale * math.log2(math.e)
    last = (G - 1) % 2

    def merge(chip):
        late_high, late_low = chunks_of(chip)[2:]
        tiles = [(1, t, len(late_high)) for t in range(NT)]
        tiles += [(0, t, len(late_low)) for t in range(NT) if late_low]
        ends = []
        if not late_low:
            ends.append(pltpu.make_async_copy(o_part.at[pl.ds(0, CH), G - 1], o_hbm.at[pl.ds(0, CH), G - 1], sem.at[G]))
            ends[0].start()
        n_pieces = 2 * len(late_high)
        keys = kv_last[0:n_pieces, 0].reshape(n_pieces * CH, D)
        vals = kv_last[0:n_pieces, 1].reshape(n_pieces * CH, D).T
        slabs = lambda x: [x[8 * i:8 * i + 8] for i in range(x.shape[0] // 8)]
        tops, sums, at = [], [], 0
        for half, t, count in tiles:
            n = 2 * CH * count
            rows = slice(half * CH + t * QT, half * CH + (t + 1) * QT)
            s = lax.dot_general(keys[:n], q_last[rows].reshape(W, D), (((1,), (1,)), ((), ())),
                                preferred_element_type=jnp.float32)
            s_s[at:at + n] = s
            top = functools.reduce(jnp.maximum, slabs(s))
            tops.append(jnp.maximum(jnp.max(top, axis=0, keepdims=True), mk[last, half, t]))
            at += n
        at = 0
        for (half, t, count), m in zip(tiles, tops):
            n = 2 * CH * count
            total = None
            for j in range(count):
                sl = slice(at + j * 2 * CH, at + (j + 1) * 2 * CH)
                p = jnp.exp2((s_s[sl] - m) * c2)
                part = functools.reduce(jnp.add, slabs(p))
                total = part if total is None else total + part
                p_s[sl] = p.astype(jnp.bfloat16)
            sums.append(jnp.sum(total, axis=0, keepdims=True))
            at += n
        at = 0
        for (half, t, count), m, total in zip(tiles, tops, sums):
            n = 2 * CH * count
            rows = slice(half * CH + t * QT, half * CH + (t + 1) * QT)
            alpha = jnp.exp2((mk[last, half, t] - m) * c2)
            inv = 1.0 / (lk[last, half, t] * alpha + total)
            acc = acck[last, half, t] * (alpha * inv) + lax.dot_general(
                vals[:, :n], p_s[at:at + n], (((1,), (0,)), ((), ())), preferred_element_type=jnp.float32) * inv
            out_s[rows] = acc.astype(jnp.bfloat16).T.reshape(QT, GQ, D)
            at += n
        for half in ((1, 0) if late_low else (1,)):
            ends.append(pltpu.make_async_copy(
                out_s.at[pl.ds(half * CH, CH)], o_hbm.at[pl.ds(half * CH, CH), G - 1], sem.at[G + 1 + half]))
            ends[-1].start()
        for c in ends:
            c.wait()

    for chip in range(4):
        @pl.when(chip_of == chip)
        def _(chip=chip):
            merge(chip)

    for c in copies:
        c.wait()


def solution(mesh):
    spec = P(('batch', 'cy', 'cx'), None, None)

    def local(q, k, v):
        t, h, d = q.shape
        kvh = k.shape[1]
        gq = h // kvh
        ch = t // 2
        ndev = mesh.shape['cy'] * mesh.shape['cx']
        w = QT * gq
        rows = 9 * 2 * ch
        any_spec = pl.BlockSpec(memory_space=pltpu.HBM)
        operands = [pltpu.with_memory_space_constraint(x, pltpu.HBM) for x in (q.reshape(t, kvh, gq, d), k, v)]
        states = [
            jax.ShapeDtypeStruct((t, kvh, gq, d), jnp.bfloat16),
            jax.ShapeDtypeStruct((t, gq, d), jnp.bfloat16),
            jax.ShapeDtypeStruct((4, 2, ch, d), jnp.bfloat16),
            jax.ShapeDtypeStruct((2, 2, NT, 1, w), jnp.float32),
            jax.ShapeDtypeStruct((2, 2, NT, 1, w), jnp.float32),
            jax.ShapeDtypeStruct((2, 2, NT, d, w), jnp.float32),
        ]
        vmem = pl.BlockSpec(memory_space=pltpu.VMEM)
        states = pl.pallas_call(
            functools.partial(kernel, scale=d ** -0.5),
            out_shape=states,
            in_specs=[any_spec] * 3,
            out_specs=[vmem] * 6,
            scratch_shapes=[
                pltpu.VMEM((kvh, t, gq, d), jnp.bfloat16),
                pltpu.VMEM((2, t, kvh, d), jnp.bfloat16),
                pltpu.VMEM((2, t * kvh, d), jnp.float32),
                pltpu.VMEM((kvh + 1, 2 * ndev, 2, ch, d), jnp.bfloat16),
                pltpu.VMEM((2, d, 12 * ch), jnp.bfloat16),
                pltpu.VMEM((2, d, 4 * ch), jnp.bfloat16),
                *[pltpu.VMEM((rows, w), jnp.float32)] * 3,
                *[pltpu.VMEM((rows, w), jnp.bfloat16)] * 3,
                *[pltpu.VMEM((4, 1, w), jnp.float32)] * 3,
                *[pltpu.VMEM((2, 1, w), jnp.float32)] * 6,
                *[pltpu.VMEM((4, 1, w), jnp.float32)] * 3,
                pltpu.SemaphoreType.DMA((3,)),
                *[pltpu.SemaphoreType.DMA((kvh,))] * 5,
            ],
            compiler_params=pltpu.CompilerParams(
                collective_id=0, has_side_effects=True, vmem_limit_bytes=40 * 2**20),
            name='ring_attention',
        )(*operands)
        out = pl.pallas_call(
            functools.partial(last_kernel, scale=d ** -0.5),
            out_shape=jax.ShapeDtypeStruct((t, kvh, gq, d), jnp.bfloat16),
            in_specs=[vmem] * 6,
            out_specs=any_spec,
            scratch_shapes=[
                pltpu.VMEM((t, gq, d), jnp.bfloat16),
                pltpu.VMEM((12 * ch, w), jnp.float32),
                pltpu.VMEM((12 * ch, w), jnp.bfloat16),
                pltpu.SemaphoreType.DMA((kvh + 3,)),
            ],
            compiler_params=pltpu.CompilerParams(vmem_limit_bytes=16 * 2**20),
            name='write_result',
        )(*states)
        return out.reshape(t, h, d)

    return jax.shard_map(local, mesh=mesh, in_specs=(spec, spec, spec), out_specs=spec, check_vma=False)
```

```python
import functools
import math

import jax
import jax.numpy as jnp
from jax import lax
from jax.experimental import pallas as pl
from jax.experimental.pallas import tpu as pltpu
from jax.sharding import PartitionSpec as P

MESH = pl.DeviceIdType.MESH
AHEAD = 3
QT = 32
NT = 3
NEG = -jnp.inf


def chunks_of(chip):
    far = 3 - chip
    early_low = [(0, j) for j in range(chip + 1) if j != far]
    late_low = [(0, far)] if far <= chip else []
    early_high = early_low + [(0, j) for j in range(chip + 1, 4) if j != far]
    early_high += [(1, j) for j in range(3, chip - 1, -1) if j != far]
    late_high = [(0, far)] + ([(1, far)] if far >= chip else [])
    return early_high, early_low, late_high, late_low


def kernel(q_hbm, k_hbm, v_hbm, o_ref, q_last, kv_last, mk, lk, acck, q_s, raw, f32s, kv, vte, vtl, *rest,
           scale):
    s_s, p_s, m_s, al_s, be_s, l_s, fin_s = (rest[3 * i:3 * i + 3] for i in range(7))
    load_sem, send_sem, xy_sem, dg_sem, se_sem, sl_sem = rest[21:]
    G, T, GQ, D = q_s.shape
    CH = T // 2
    C2 = 2 * CH
    W = QT * GQ
    cb = lax.axis_index('batch')
    cy = lax.axis_index('cy')
    cx = lax.axis_index('cx')
    ox = lax.rem(cx + 2, 4)
    sx = cx + 1 - 2 * lax.rem(cx, 2)
    oy = 1 - cy
    x_dev = (cb, cy, ox)
    y_dev = (cb, oy, cx)
    s_dev = (cb, cy, sx)
    me = cy * 4 + cx
    rx, ry, rd = cy * 4 + ox, oy * 4 + cx, oy * 4 + ox
    odd = lax.rem(cx, 2)
    chip_of = me // 2

    kcopy = pltpu.make_async_copy(k_hbm, raw.at[0], load_sem.at[0])
    vcopy = pltpu.make_async_copy(v_hbm, raw.at[1], load_sem.at[1])
    kcopy.start()
    vcopy.start()

    barrier = pltpu.get_barrier_semaphore()
    for dev in (x_dev, y_dev, s_dev):
        pl.semaphore_signal(barrier, inc=1, device_id=dev, device_id_type=MESH)

    for g in range(G):
        pltpu.make_async_copy(q_hbm.at[:, g], q_s.at[g], load_sem.at[2]).start()

    def take(g):
        for which in (0, 1):
            rows = f32s[which, pl.ds(g, T, stride=G), :].astype(jnp.bfloat16)
            kv[g, 2 * me, which] = rows[:CH]
            kv[g, 2 * me + 1, which] = rows[CH:]

    for which, copy in ((0, kcopy), (1, vcopy)):
        copy.wait()
        f32s[which] = raw[which].astype(jnp.float32).reshape(T * G, D)
    for g in range(AHEAD):
        take(g)

    pl.semaphore_wait(barrier, 3)

    def piece(g, r, full):
        return kv.at[g, pl.ds(2 * r, 2)] if full else kv.at[g, 2 * r]

    def send(g, ref, recv_sem, dev):
        pltpu.make_async_remote_copy(
            src_ref=ref, dst_ref=ref, send_sem=send_sem.at[g], recv_sem=recv_sem.at[g],
            device_id=dev, device_id_type=MESH).start()

    def arrived(g, count, recv_sem):
        ref = kv.at[g, 0:count]
        pltpu.make_async_remote_copy(
            src_ref=ref, dst_ref=ref, send_sem=send_sem.at[g], recv_sem=recv_sem.at[g],
            device_id=x_dev, device_id_type=MESH).wait_recv()

    c2 = scale * math.log2(math.e)
    sub = lax.broadcasted_iota(jnp.int32, (8, W), 0)
    base = sub - lax.broadcasted_iota(jnp.int32, (8, W), 1) // GQ

    def keys(g, chunk_list, which):
        parts = [kv[g, 4 * j + half + 2 * core, which] for half, j in chunk_list for core in (0, 1)]
        return jnp.concatenate(parts, axis=0)

    def pipeline(chip):
        xc, yc, far = chip ^ 1, chip ^ 2, chip ^ 3
        own_x, own_y = True, True
        got_x, got_y, got_far = True, True, True
        cross_high = True
        n_xy = 2 + got_x + got_y
        n_far = 1 + got_far
        n_sent = (2 + own_x + own_y) + 2 + (1 + cross_high) + (2 + got_x + got_y) + n_far

        def start_own(g):
            send(g, piece(g, me, own_x), xy_sem, x_dev)
            send(g, piece(g, me, own_y), xy_sem, y_dev)
            send(g, piece(g, me, True), se_sem, s_dev)

        def forward(g):
            arrived(g, n_xy, xy_sem)
            send(g, kv.at[g, 2 * rx], dg_sem, y_dev)
            if cross_high:
                send(g, kv.at[g, 2 * ry + 1], dg_sem, x_dev)
            send(g, piece(g, rx, got_x), se_sem, s_dev)
            send(g, piece(g, ry, got_y), se_sem, s_dev)

        def diagonal(g):
            arrived(g, n_far, dg_sem)
            send(g, piece(g, rd, got_far), sl_sem, s_dev)

        for g in range(AHEAD):
            start_own(g)
        for g in range(AHEAD, G):
            take(g)
        pltpu.make_async_copy(q_s, q_s, load_sem.at[2]).wait()
        q_last[...] = q_s[G - 1]

        lists = chunks_of(chip)
        names = ('eh', 'el', 'lh', 'll')
        rows = {}
        at = 0
        for name, lst in zip(names, lists):
            rows[name] = (at, C2 * len(lst))
            at += C2 * len(lst)
        lst = dict(zip(names, lists))
        halves = (1, 0)

        def transposed(g, slot, names):
            for name, ref in names:
                n = rows[name][1]
                ref[slot, :, :n] = keys(g, lst[name], 1).T

        def split(u):
            return lax.div(u + NT, NT) - 1, lax.rem(u + NT, NT)

        def score(g, t, half, name, slot, masked):
            at, n = rows[name]
            qv = q_s[g, pl.ds(half * CH + t * QT, QT)].reshape(W, D)
            s = lax.dot_general(keys(g, lst[name], 0), qv, (((1,), (1,)), ((), ())),
                                preferred_element_type=jnp.float32)
            edge = n - C2 if masked else n
            top = None
            if edge:
                s_s[slot][at:at + edge] = s[:edge]
                for i in range(edge // 8):
                    si = s[8 * i:8 * i + 8]
                    top = si if top is None else jnp.maximum(top, si)
            if masked:
                thr = t * QT + CH * (odd if half == 0 else -odd)
                for i in range(C2 // 8):
                    first = 8 * i if (half == 0 or i < CH // 8) else 8 * i - C2
                    si = jnp.where(base <= thr - first, s[edge + 8 * i:edge + 8 * i + 8], NEG)
                    s_s[slot][at + edge + 8 * i:at + edge + 8 * i + 8] = si
                    top = si if top is None else jnp.maximum(top, si)
            return jnp.max(top, axis=0, keepdims=True)

        def stage_a(u, slot, early=True, late=True):
            g, t = split(u)
            par = lax.rem(g + 2, 2)
            gl = jnp.where(g < 2, G, g - 2)
            ql = jnp.maximum(g - 2, 0)
            for half in halves:
                e, l = ('eh', 'lh') if half else ('el', 'll')
                if late and lst[l]:
                    old = mk[par, half, t]
                    m = jnp.maximum(score_late(gl, ql, t, half, l, slot), old)
                    m_s[slot][2 + half] = m
                    al_s[slot][half] = jnp.exp2((old - m) * c2)
                if early:
                    m = score(g, t, half, e, slot, True)
                    m_s[slot][half] = m
                    mk[par, half, t] = m

        def score_late(gl, ql, t, half, name, slot):
            at, n = rows[name]
            qv = q_s[ql, pl.ds(half * CH + t * QT, QT)].reshape(W, D)
            s = lax.dot_general(keys(gl, lst[name], 0), qv, (((1,), (1,)), ((), ())),
                                preferred_element_type=jnp.float32)
            s_s[slot][at:at + n] = s
            top = s[:8]
            for i in range(1, n // 8):
                top = jnp.maximum(top, s[8 * i:8 * i + 8])
            return jnp.max(top, axis=0, keepdims=True)

        def weights(name, slot, m):
            at, n = rows[name]
            total = None
            for j in range(n // C2):
                sl = slice(at + j * C2, at + (j + 1) * C2)
                p = jnp.exp2((s_s[slot][sl] - m) * c2)
                for i in range(C2 // 8):
                    pi = p[8 * i:8 * i + 8]
                    total = pi if total is None else total + pi
                p_s[slot][sl] = p.astype(jnp.bfloat16)
            return jnp.sum(total, axis=0, keepdims=True)

        def stage_b(u, slot, early=True, late=True):
            g, t = split(u)
            par = lax.rem(g + 2, 2)
            for half in halves:
                e, l = ('eh', 'lh') if half else ('el', 'll')
                if late and lst[l]:
                    total = weights(l, slot, m_s[slot][2 + half])
                    l_s[slot][2 + half] = lk[par, half, t] * al_s[slot][half] + total
                    be_s[slot][half] = al_s[slot][half]
                if early:
                    total = weights(e, slot, m_s[slot][half])
                    l_s[slot][half] = total
                    lk[par, half, t] = total

        def values(name, ref, par, slot):
            at, n = rows[name]
            return lax.dot_general(ref[par, :, :n], p_s[slot][at:at + n], (((1,), (0,)), ((), ())),
                                   preferred_element_type=jnp.float32)

        def put(slot, half, acc, total):
            fin_s[slot][half] = (acc * (1.0 / total)).astype(jnp.bfloat16)

        def stage_d(u, slot, late_only=False):
            g, t = split(u)
            for half in halves:
                late = bool(lst['lh' if half else 'll'])
                if late or not late_only:
                    to = jnp.maximum(g - 2, 0) if late else jnp.maximum(g, 0)
                    o_ref[pl.ds(half * CH + t * QT, QT), to] = fin_s[slot][half].T.reshape(QT, GQ, D)

        def stage_c(u, slot, early=True, late=True):
            g, t = split(u)
            par = lax.rem(g + 2, 2)
            ge = jnp.maximum(g, 0)
            gl = jnp.maximum(g - 2, 0)
            for half in halves:
                e, l = ('eh', 'lh') if half else ('el', 'll')
                if late and lst[l]:
                    acc = acck[par, half, t] * be_s[slot][half] + values(l, vtl, lax.rem(gl, 2), slot)
                    put(slot, half, acc, l_s[slot][2 + half])
                if early:
                    acc = values(e, vte, lax.rem(ge, 2), slot)
                    if lst[l]:
                        acck[par, half, t] = acc
                    else:
                        put(slot, half, acc, l_s[slot][half])

        def service(g):
            arrived(g, 2 + n_xy, se_sem)

            @pl.when(g > 1)
            def _():
                arrived(g - 2, n_far, sl_sem)
                transposed(g - 2, lax.rem(g, 2), (('lh', vtl),))
            transposed(g, lax.rem(g, 2), (('eh', vte),))

        n = NT * G
        forward(0)
        start_own(AHEAD)

        def body(pair, carry):
            for odd_i in (0, 1):
                i = 2 * pair + odd_i

                @pl.when(lax.rem(i, NT) == 0)
                def _(i=i):
                    service(lax.div(i, NT))

                @pl.when(jnp.logical_and(lax.rem(i, NT) == 1, i < n - NT))
                def _(i=i):
                    forward(lax.div(i, NT) + 1)

                @pl.when(jnp.logical_and(lax.rem(i, NT) == 1, i < n - NT - NT * AHEAD))
                def _(i=i):
                    start_own(lax.div(i, NT) + 1 + AHEAD)

                @pl.when(jnp.logical_and(lax.rem(i, NT) == 2, i >= NT))
                def _(i=i):
                    diagonal(lax.div(i, NT) - 1)

                stage_a(i, odd_i)
                stage_b(i - 1, 1 - odd_i)
                stage_c(i - 1, 1 - odd_i)
                stage_d(i - 2, odd_i)
            return carry

        lax.fori_loop(0, n // 2, body, 0)
        diagonal(G - 1)
        stage_b(n - 1, 1 - n % 2)
        stage_c(n - 1, 1 - n % 2)
        stage_d(n - 2, n % 2)
        stage_d(n - 1, 1 - n % 2)

        arrived(G - 2, n_far, sl_sem)
        transposed(G - 2, G % 2, (('lh', vtl),))
        for t in range(NT):
            stage_a(n + t, t, early=False)
        for t in range(NT):
            stage_b(n + t, t, early=False)
        for t in range(NT):
            stage_c(n + t, t, early=False)
            stage_d(n + t, t, late_only=True)
        arrived(G - 1, n_far, sl_sem)
        for i, (half, j) in enumerate(lst['lh']):
            for core in (0, 1):
                kv_last[2 * i + core] = kv[G - 1, 4 * j + half + 2 * core]

        def drain(g, carry):
            ref = kv.at[g, 0:n_sent]
            pltpu.make_async_remote_copy(
                src_ref=ref, dst_ref=ref, send_sem=send_sem.at[g], recv_sem=xy_sem.at[g],
                device_id=x_dev, device_id_type=MESH).wait_send()
            return carry

        lax.fori_loop(0, G, drain, 0)

    for chip in range(4):
        @pl.when(chip_of == chip)
        def _(chip=chip):
            pipeline(chip)


def last_kernel(o_part, q_last, kv_last, mk, lk, acck, o_hbm, out_s, s_s, p_s, sem, *, scale):
    T, G, GQ, D = o_part.shape
    CH = T // 2
    W = QT * GQ
    chip_of = lax.axis_index('cy') * 2 + lax.axis_index('cx') // 2
    step = T // 4
    copies = [pltpu.make_async_copy(o_part.at[pl.ds(i * step, step), pl.ds(0, G - 1)],
                                    o_hbm.at[pl.ds(i * step, step), pl.ds(0, G - 1)], sem.at[i]) for i in range(4)]
    for c in copies:
        c.start()
    c2 = scale * math.log2(math.e)
    last = (G - 1) % 2

    def merge(chip):
        late_high, late_low = chunks_of(chip)[2:]
        tiles = [(1, t, len(late_high)) for t in range(NT)]
        tiles += [(0, t, len(late_low)) for t in range(NT) if late_low]
        ends = []
        if not late_low:
            ends.append(pltpu.make_async_copy(o_part.at[pl.ds(0, CH), G - 1], o_hbm.at[pl.ds(0, CH), G - 1], sem.at[G]))
            ends[0].start()
        n_pieces = 2 * len(late_high)
        keys = kv_last[0:n_pieces, 0].reshape(n_pieces * CH, D)
        vals = kv_last[0:n_pieces, 1].reshape(n_pieces * CH, D).T
        slabs = lambda x: [x[8 * i:8 * i + 8] for i in range(x.shape[0] // 8)]
        tops, sums, at = [], [], 0
        for half, t, count in tiles:
            n = 2 * CH * count
            rows = slice(half * CH + t * QT, half * CH + (t + 1) * QT)
            s = lax.dot_general(keys[:n], q_last[rows].reshape(W, D), (((1,), (1,)), ((), ())),
                                preferred_element_type=jnp.float32)
            s_s[at:at + n] = s
            top = functools.reduce(jnp.maximum, slabs(s))
            tops.append(jnp.maximum(jnp.max(top, axis=0, keepdims=True), mk[last, half, t]))
            at += n
        at = 0
        for (half, t, count), m in zip(tiles, tops):
            n = 2 * CH * count
            total = None
            for j in range(count):
                sl = slice(at + j * 2 * CH, at + (j + 1) * 2 * CH)
                p = jnp.exp2((s_s[sl] - m) * c2)
                part = functools.reduce(jnp.add, slabs(p))
                total = part if total is None else total + part
                p_s[sl] = p.astype(jnp.bfloat16)
            sums.append(jnp.sum(total, axis=0, keepdims=True))
            at += n
        at = 0
        for (half, t, count), m, total in zip(tiles, tops, sums):
            n = 2 * CH * count
            rows = slice(half * CH + t * QT, half * CH + (t + 1) * QT)
            alpha = jnp.exp2((mk[last, half, t] - m) * c2)
            inv = 1.0 / (lk[last, half, t] * alpha + total)
            acc = acck[last, half, t] * (alpha * inv) + lax.dot_general(
                vals[:, :n], p_s[at:at + n], (((1,), (0,)), ((), ())), preferred_element_type=jnp.float32) * inv
            out_s[rows] = acc.astype(jnp.bfloat16).T.reshape(QT, GQ, D)
            at += n
        for half in ((1, 0) if late_low else (1,)):
            ends.append(pltpu.make_async_copy(
                out_s.at[pl.ds(half * CH, CH)], o_hbm.at[pl.ds(half * CH, CH), G - 1], sem.at[G + 1 + half]))
            ends[-1].start()
        for c in ends:
            c.wait()

    for chip in range(4):
        @pl.when(chip_of == chip)
        def _(chip=chip):
            merge(chip)

    for c in copies:
        c.wait()


def solution(mesh):
    spec = P(('batch', 'cy', 'cx'), None, None)

    def local(q, k, v):
        t, h, d = q.shape
        kvh = k.shape[1]
        gq = h // kvh
        ch = t // 2
        ndev = mesh.shape['cy'] * mesh.shape['cx']
        w = QT * gq
        rows = 9 * 2 * ch
        any_spec = pl.BlockSpec(memory_space=pltpu.HBM)
        operands = [pltpu.with_memory_space_constraint(x, pltpu.HBM) for x in (q.reshape(t, kvh, gq, d), k, v)]
        states = [
            jax.ShapeDtypeStruct((t, kvh, gq, d), jnp.bfloat16),
            jax.ShapeDtypeStruct((t, gq, d), jnp.bfloat16),
            jax.ShapeDtypeStruct((4, 2, ch, d), jnp.bfloat16),
            jax.ShapeDtypeStruct((2, 2, NT, 1, w), jnp.float32),
            jax.ShapeDtypeStruct((2, 2, NT, 1, w), jnp.float32),
            jax.ShapeDtypeStruct((2, 2, NT, d, w), jnp.float32),
        ]
        vmem = pl.BlockSpec(memory_space=pltpu.VMEM)
        states = pl.pallas_call(
            functools.partial(kernel, scale=d ** -0.5),
            out_shape=states,
            in_specs=[any_spec] * 3,
            out_specs=[vmem] * 6,
            scratch_shapes=[
                pltpu.VMEM((kvh, t, gq, d), jnp.bfloat16),
                pltpu.VMEM((2, t, kvh, d), jnp.bfloat16),
                pltpu.VMEM((2, t * kvh, d), jnp.float32),
                pltpu.VMEM((kvh + 1, 2 * ndev, 2, ch, d), jnp.bfloat16),
                pltpu.VMEM((2, d, 12 * ch), jnp.bfloat16),
                pltpu.VMEM((2, d, 4 * ch), jnp.bfloat16),
                *[pltpu.VMEM((rows, w), jnp.float32)] * 3,
                *[pltpu.VMEM((rows, w), jnp.bfloat16)] * 3,
                *[pltpu.VMEM((4, 1, w), jnp.float32)] * 3,
                *[pltpu.VMEM((2, 1, w), jnp.float32)] * 6,
                *[pltpu.VMEM((4, 1, w), jnp.float32)] * 3,
                *[pltpu.VMEM((2, d, w), jnp.bfloat16)] * 3,
                pltpu.SemaphoreType.DMA((3,)),
                *[pltpu.SemaphoreType.DMA((kvh,))] * 5,
            ],
            compiler_params=pltpu.CompilerParams(
                collective_id=0, has_side_effects=True, vmem_limit_bytes=40 * 2**20),
            name='ring_attention',
        )(*operands)
        out = pl.pallas_call(
            functools.partial(last_kernel, scale=d ** -0.5),
            out_shape=jax.ShapeDtypeStruct((t, kvh, gq, d), jnp.bfloat16),
            in_specs=[vmem] * 6,
            out_specs=any_spec,
            scratch_shapes=[
                pltpu.VMEM((t, gq, d), jnp.bfloat16),
                pltpu.VMEM((12 * ch, w), jnp.float32),
                pltpu.VMEM((12 * ch, w), jnp.bfloat16),
                pltpu.SemaphoreType.DMA((kvh + 3,)),
            ],
            compiler_params=pltpu.CompilerParams(vmem_limit_bytes=16 * 2**20),
            name='write_result',
        )(*states)
        return out.reshape(t, h, d)

    return jax.shard_map(local, mesh=mesh, in_specs=(spec, spec, spec), out_specs=spec, check_vma=False)
```

```python
import functools
import math

import jax
import jax.numpy as jnp
from jax import lax
from jax.experimental import pallas as pl
from jax.experimental.pallas import tpu as pltpu
from jax.sharding import PartitionSpec as P

MESH = pl.DeviceIdType.MESH
AHEAD = 3
QT = 32
NT = 3
NEG = -jnp.inf


def chunks_of(chip):
    far = 3 - chip
    early_low = [(0, j) for j in range(chip + 1) if j != far]
    late_low = [(0, far)] if far <= chip else []
    early_high = early_low + [(0, j) for j in range(chip + 1, 4) if j != far]
    early_high += [(1, j) for j in range(3, chip - 1, -1) if j != far]
    late_high = [(0, far)] + ([(1, far)] if far >= chip else [])
    return early_high, early_low, late_high, late_low


def kernel(q_hbm, k_hbm, v_hbm, o_ref, q_last, kv_last, mk, lk, acck, q_s, raw, f32s, kv, vte, vtl, *rest,
           scale):
    s_s, p_s, m_s, al_s, be_s, l_s, fin_s = (rest[3 * i:3 * i + 3] for i in range(7))
    load_sem, send_sem, xy_sem, dg_sem, se_sem, sl_sem = rest[21:]
    G, T, GQ, D = q_s.shape
    CH = T // 2
    C2 = 2 * CH
    W = QT * GQ
    cb = lax.axis_index('batch')
    cy = lax.axis_index('cy')
    cx = lax.axis_index('cx')
    ox = lax.rem(cx + 2, 4)
    sx = cx + 1 - 2 * lax.rem(cx, 2)
    oy = 1 - cy
    x_dev = (cb, cy, ox)
    y_dev = (cb, oy, cx)
    s_dev = (cb, cy, sx)
    me = cy * 4 + cx
    rx, ry, rd = cy * 4 + ox, oy * 4 + cx, oy * 4 + ox
    odd = lax.rem(cx, 2)
    chip_of = me // 2

    kcopy = pltpu.make_async_copy(k_hbm, raw.at[0], load_sem.at[0])
    vcopy = pltpu.make_async_copy(v_hbm, raw.at[1], load_sem.at[1])
    kcopy.start()
    vcopy.start()

    barrier = pltpu.get_barrier_semaphore()
    for dev in (x_dev, y_dev, s_dev):
        pl.semaphore_signal(barrier, inc=1, device_id=dev, device_id_type=MESH)

    for g in range(G):
        pltpu.make_async_copy(q_hbm.at[:, g], q_s.at[g], load_sem.at[2]).start()

    def take(g):
        for which in (0, 1):
            rows = f32s[which, pl.ds(g, T, stride=G), :].astype(jnp.bfloat16)
            kv[g, 2 * me, which] = rows[:CH]
            kv[g, 2 * me + 1, which] = rows[CH:]

    for which, copy in ((0, kcopy), (1, vcopy)):
        copy.wait()
        f32s[which] = raw[which].astype(jnp.float32).reshape(T * G, D)
    for g in range(AHEAD):
        take(g)

    pl.semaphore_wait(barrier, 3)

    def piece(g, r, full):
        return kv.at[g, pl.ds(2 * r, 2)] if full else kv.at[g, 2 * r]

    def send(g, ref, recv_sem, dev):
        pltpu.make_async_remote_copy(
            src_ref=ref, dst_ref=ref, send_sem=send_sem.at[0], recv_sem=recv_sem.at[g],
            device_id=dev, device_id_type=MESH).start()

    def arrived(g, count, recv_sem):
        ref = kv.at[g, 0:count]
        pltpu.make_async_remote_copy(
            src_ref=ref, dst_ref=ref, send_sem=send_sem.at[0], recv_sem=recv_sem.at[g],
            device_id=x_dev, device_id_type=MESH).wait_recv()

    c2 = scale * math.log2(math.e)
    sub = lax.broadcasted_iota(jnp.int32, (8, W), 0)
    base = sub - lax.broadcasted_iota(jnp.int32, (8, W), 1) // GQ

    def keys(g, chunk_list, which):
        parts = [kv[g, 4 * j + half + 2 * core, which] for half, j in chunk_list for core in (0, 1)]
        return jnp.concatenate(parts, axis=0)

    def pipeline(chip):
        xc, yc, far = chip ^ 1, chip ^ 2, chip ^ 3
        own_x, own_y = True, True
        got_x, got_y, got_far = True, True, True
        cross_high = True
        n_xy = 2 + got_x + got_y
        n_far = 1 + got_far
        n_sent = (2 + own_x + own_y) + 2 + (1 + cross_high) + (2 + got_x + got_y) + n_far

        def start_own(g):
            send(g, piece(g, me, own_x), xy_sem, x_dev)
            send(g, piece(g, me, own_y), xy_sem, y_dev)
            send(g, piece(g, me, True), se_sem, s_dev)

        def forward(g):
            arrived(g, n_xy, xy_sem)
            send(g, kv.at[g, 2 * rx], dg_sem, y_dev)
            if cross_high:
                send(g, kv.at[g, 2 * ry + 1], dg_sem, x_dev)
            send(g, piece(g, rx, got_x), se_sem, s_dev)
            send(g, piece(g, ry, got_y), se_sem, s_dev)

        def diagonal(g):
            arrived(g, n_far, dg_sem)
            send(g, piece(g, rd, got_far), sl_sem, s_dev)

        for g in range(AHEAD):
            start_own(g)
        for g in range(AHEAD, G):
            take(g)
        pltpu.make_async_copy(q_s, q_s, load_sem.at[2]).wait()
        q_last[...] = q_s[G - 1]

        lists = chunks_of(chip)
        names = ('eh', 'el', 'lh', 'll')
        rows = {}
        at = 0
        for name, lst in zip(names, lists):
            rows[name] = (at, C2 * len(lst))
            at += C2 * len(lst)
        lst = dict(zip(names, lists))
        halves = (1, 0)

        def transposed(g, slot, names):
            for name, ref in names:
                n = rows[name][1]
                ref[slot, :, :n] = keys(g, lst[name], 1).T

        def split(u):
            return lax.div(u + NT, NT) - 1, lax.rem(u + NT, NT)

        def score(g, t, half, name, slot, masked):
            at, n = rows[name]
            qv = q_s[g, pl.ds(half * CH + t * QT, QT)].reshape(W, D)
            s = lax.dot_general(keys(g, lst[name], 0), qv, (((1,), (1,)), ((), ())),
                                preferred_element_type=jnp.float32)
            edge = n - C2 if masked else n
            top = None
            if edge:
                s_s[slot][at:at + edge] = s[:edge]
                for i in range(edge // 8):
                    si = s[8 * i:8 * i + 8]
                    top = si if top is None else jnp.maximum(top, si)
            if masked:
                thr = t * QT + CH * (odd if half == 0 else -odd)
                for i in range(C2 // 8):
                    first = 8 * i if (half == 0 or i < CH // 8) else 8 * i - C2
                    si = jnp.where(base <= thr - first, s[edge + 8 * i:edge + 8 * i + 8], NEG)
                    s_s[slot][at + edge + 8 * i:at + edge + 8 * i + 8] = si
                    top = si if top is None else jnp.maximum(top, si)
            return jnp.max(top, axis=0, keepdims=True)

        def stage_a(u, slot, early=True, late=True):
            g, t = split(u)
            par = lax.rem(g + 2, 2)
            gl = jnp.where(g < 2, G, g - 2)
            ql = jnp.maximum(g - 2, 0)
            for half in halves:
                e, l = ('eh', 'lh') if half else ('el', 'll')
                if late and lst[l]:
                    old = mk[par, half, t]
                    m = jnp.maximum(score_late(gl, ql, t, half, l, slot), old)
                    m_s[slot][2 + half] = m
                    al_s[slot][half] = jnp.exp2((old - m) * c2)
                if early:
                    m = score(g, t, half, e, slot, True)
                    m_s[slot][half] = m
                    mk[par, half, t] = m

        def score_late(gl, ql, t, half, name, slot):
            at, n = rows[name]
            qv = q_s[ql, pl.ds(half * CH + t * QT, QT)].reshape(W, D)
            s = lax.dot_general(keys(gl, lst[name], 0), qv, (((1,), (1,)), ((), ())),
                                preferred_element_type=jnp.float32)
            s_s[slot][at:at + n] = s
            top = s[:8]
            for i in range(1, n // 8):
                top = jnp.maximum(top, s[8 * i:8 * i + 8])
            return jnp.max(top, axis=0, keepdims=True)

        def weights(name, slot, m):
            at, n = rows[name]
            total = None
            for j in range(n // C2):
                sl = slice(at + j * C2, at + (j + 1) * C2)
                p = jnp.exp2((s_s[slot][sl] - m) * c2)
                for i in range(C2 // 8):
                    pi = p[8 * i:8 * i + 8]
                    total = pi if total is None else total + pi
                p_s[slot][sl] = p.astype(jnp.bfloat16)
            return jnp.sum(total, axis=0, keepdims=True)

        def stage_b(u, slot, early=True, late=True):
            g, t = split(u)
            par = lax.rem(g + 2, 2)
            for half in halves:
                e, l = ('eh', 'lh') if half else ('el', 'll')
                if late and lst[l]:
                    total = weights(l, slot, m_s[slot][2 + half])
                    l_s[slot][2 + half] = lk[par, half, t] * al_s[slot][half] + total
                    be_s[slot][half] = al_s[slot][half]
                if early:
                    total = weights(e, slot, m_s[slot][half])
                    l_s[slot][half] = total
                    lk[par, half, t] = total

        def values(name, ref, par, slot):
            at, n = rows[name]
            return lax.dot_general(ref[par, :, :n], p_s[slot][at:at + n], (((1,), (0,)), ((), ())),
                                   preferred_element_type=jnp.float32)

        def put(slot, half, acc, total):
            fin_s[slot][half] = (acc * (1.0 / total)).astype(jnp.bfloat16)

        def stage_d(u, slot, late_only=False):
            g, t = split(u)
            for half in halves:
                late = bool(lst['lh' if half else 'll'])
                if late or not late_only:
                    to = jnp.maximum(g - 2, 0) if late else jnp.maximum(g, 0)
                    o_ref[pl.ds(half * CH + t * QT, QT), to] = fin_s[slot][half].T.reshape(QT, GQ, D)

        def stage_c(u, slot, early=True, late=True):
            g, t = split(u)
            par = lax.rem(g + 2, 2)
            ge = jnp.maximum(g, 0)
            gl = jnp.maximum(g - 2, 0)
            for half in halves:
                e, l = ('eh', 'lh') if half else ('el', 'll')
                if late and lst[l]:
                    acc = acck[par, half, t] * be_s[slot][half] + values(l, vtl, lax.rem(gl, 2), slot)
                    put(slot, half, acc, l_s[slot][2 + half])
                if early:
                    acc = values(e, vte, lax.rem(ge, 2), slot)
                    if lst[l]:
                        acck[par, half, t] = acc
                    else:
                        put(slot, half, acc, l_s[slot][half])

        def service(g):
            arrived(g, 2 + n_xy, se_sem)

            @pl.when(g > 1)
            def _():
                arrived(g - 2, n_far, sl_sem)
                transposed(g - 2, lax.rem(g, 2), (('lh', vtl),))
            transposed(g, lax.rem(g, 2), (('eh', vte),))

        n = NT * G
        forward(0)
        start_own(AHEAD)

        def body(pair, carry):
            for odd_i in (0, 1):
                i = 2 * pair + odd_i

                @pl.when(lax.rem(i, NT) == 0)
                def _(i=i):
                    service(lax.div(i, NT))

                @pl.when(jnp.logical_and(lax.rem(i, NT) == 1, i < n - NT))
                def _(i=i):
                    forward(lax.div(i, NT) + 1)

                @pl.when(jnp.logical_and(lax.rem(i, NT) == 2, i < n - NT - NT * AHEAD))
                def _(i=i):
                    start_own(lax.div(i, NT) + 1 + AHEAD)

                @pl.when(jnp.logical_and(lax.rem(i, NT) == 2, i >= NT))
                def _(i=i):
                    diagonal(lax.div(i, NT) - 1)

                stage_a(i, odd_i)
                stage_b(i - 1, 1 - odd_i)
                stage_c(i - 1, 1 - odd_i)
                stage_d(i - 2, odd_i)
            return carry

        lax.fori_loop(0, n // 2, body, 0)
        diagonal(G - 1)
        stage_b(n - 1, 1 - n % 2)
        stage_c(n - 1, 1 - n % 2)
        stage_d(n - 2, n % 2)
        stage_d(n - 1, 1 - n % 2)

        arrived(G - 2, n_far, sl_sem)
        transposed(G - 2, G % 2, (('lh', vtl),))
        for t in range(NT):
            stage_a(n + t, t, early=False)
        for t in range(NT):
            stage_b(n + t, t, early=False)
        for t in range(NT):
            stage_c(n + t, t, early=False)
            stage_d(n + t, t, late_only=True)
        arrived(G - 1, n_far, sl_sem)
        for i, (half, j) in enumerate(lst['lh']):
            for core in (0, 1):
                kv_last[2 * i + core] = kv[G - 1, 4 * j + half + 2 * core]

        ref = kv.at[0:G, 0:n_sent]
        pltpu.make_async_remote_copy(
            src_ref=ref, dst_ref=ref, send_sem=send_sem.at[0], recv_sem=xy_sem.at[0],
            device_id=x_dev, device_id_type=MESH).wait_send()

    for chip in range(4):
        @pl.when(chip_of == chip)
        def _(chip=chip):
            pipeline(chip)


def last_kernel(o_part, q_last, kv_last, mk, lk, acck, o_hbm, out_s, s_s, p_s, sem, *, scale):
    T, G, GQ, D = o_part.shape
    CH = T // 2
    W = QT * GQ
    chip_of = lax.axis_index('cy') * 2 + lax.axis_index('cx') // 2
    step = T // 4
    copies = [pltpu.make_async_copy(o_part.at[pl.ds(i * step, step), pl.ds(0, G - 1)],
                                    o_hbm.at[pl.ds(i * step, step), pl.ds(0, G - 1)], sem.at[i]) for i in range(4)]
    for c in copies:
        c.start()
    c2 = scale * math.log2(math.e)
    last = (G - 1) % 2

    def merge(chip):
        late_high, late_low = chunks_of(chip)[2:]
        tiles = [(1, t, len(late_high)) for t in range(NT)]
        tiles += [(0, t, len(late_low)) for t in range(NT) if late_low]
        ends = []
        if not late_low:
            ends.append(pltpu.make_async_copy(o_part.at[pl.ds(0, CH), G - 1], o_hbm.at[pl.ds(0, CH), G - 1], sem.at[G]))
            ends[0].start()
        n_pieces = 2 * len(late_high)
        keys = kv_last[0:n_pieces, 0].reshape(n_pieces * CH, D)
        vals = kv_last[0:n_pieces, 1].reshape(n_pieces * CH, D).T
        slabs = lambda x: [x[8 * i:8 * i + 8] for i in range(x.shape[0] // 8)]
        tops, sums, at = [], [], 0
        for half, t, count in tiles:
            n = 2 * CH * count
            rows = slice(half * CH + t * QT, half * CH + (t + 1) * QT)
            s = lax.dot_general(keys[:n], q_last[rows].reshape(W, D), (((1,), (1,)), ((), ())),
                                preferred_element_type=jnp.float32)
            s_s[at:at + n] = s
            top = functools.reduce(jnp.maximum, slabs(s))
            tops.append(jnp.maximum(jnp.max(top, axis=0, keepdims=True), mk[last, half, t]))
            at += n
        at = 0
        for (half, t, count), m in zip(tiles, tops):
            n = 2 * CH * count
            total = None
            for j in range(count):
                sl = slice(at + j * 2 * CH, at + (j + 1) * 2 * CH)
                p = jnp.exp2((s_s[sl] - m) * c2)
                part = functools.reduce(jnp.add, slabs(p))
                total = part if total is None else total + part
                p_s[sl] = p.astype(jnp.bfloat16)
            sums.append(jnp.sum(total, axis=0, keepdims=True))
            at += n
        at = 0
        for (half, t, count), m, total in zip(tiles, tops, sums):
            n = 2 * CH * count
            rows = slice(half * CH + t * QT, half * CH + (t + 1) * QT)
            alpha = jnp.exp2((mk[last, half, t] - m) * c2)
            inv = 1.0 / (lk[last, half, t] * alpha + total)
            acc = acck[last, half, t] * (alpha * inv) + lax.dot_general(
                vals[:, :n], p_s[at:at + n], (((1,), (0,)), ((), ())), preferred_element_type=jnp.float32) * inv
            out_s[rows] = acc.astype(jnp.bfloat16).T.reshape(QT, GQ, D)
            at += n
        for half in ((1, 0) if late_low else (1,)):
            ends.append(pltpu.make_async_copy(
                out_s.at[pl.ds(half * CH, CH)], o_hbm.at[pl.ds(half * CH, CH), G - 1], sem.at[G + 1 + half]))
            ends[-1].start()
        for c in ends:
            c.wait()

    for chip in range(4):
        @pl.when(chip_of == chip)
        def _(chip=chip):
            merge(chip)

    for c in copies:
        c.wait()


def solution(mesh):
    spec = P(('batch', 'cy', 'cx'), None, None)

    def local(q, k, v):
        t, h, d = q.shape
        kvh = k.shape[1]
        gq = h // kvh
        ch = t // 2
        ndev = mesh.shape['cy'] * mesh.shape['cx']
        w = QT * gq
        rows = 9 * 2 * ch
        any_spec = pl.BlockSpec(memory_space=pltpu.HBM)
        operands = [pltpu.with_memory_space_constraint(x, pltpu.HBM) for x in (q.reshape(t, kvh, gq, d), k, v)]
        states = [
            jax.ShapeDtypeStruct((t, kvh, gq, d), jnp.bfloat16),
            jax.ShapeDtypeStruct((t, gq, d), jnp.bfloat16),
            jax.ShapeDtypeStruct((4, 2, ch, d), jnp.bfloat16),
            jax.ShapeDtypeStruct((2, 2, NT, 1, w), jnp.float32),
            jax.ShapeDtypeStruct((2, 2, NT, 1, w), jnp.float32),
            jax.ShapeDtypeStruct((2, 2, NT, d, w), jnp.float32),
        ]
        vmem = pl.BlockSpec(memory_space=pltpu.VMEM)
        states = pl.pallas_call(
            functools.partial(kernel, scale=d ** -0.5),
            out_shape=states,
            in_specs=[any_spec] * 3,
            out_specs=[vmem] * 6,
            scratch_shapes=[
                pltpu.VMEM((kvh, t, gq, d), jnp.bfloat16),
                pltpu.VMEM((2, t, kvh, d), jnp.bfloat16),
                pltpu.VMEM((2, t * kvh, d), jnp.float32),
                pltpu.VMEM((kvh + 1, 2 * ndev, 2, ch, d), jnp.bfloat16),
                pltpu.VMEM((2, d, 12 * ch), jnp.bfloat16),
                pltpu.VMEM((2, d, 4 * ch), jnp.bfloat16),
                *[pltpu.VMEM((rows, w), jnp.float32)] * 3,
                *[pltpu.VMEM((rows, w), jnp.bfloat16)] * 3,
                *[pltpu.VMEM((4, 1, w), jnp.float32)] * 3,
                *[pltpu.VMEM((2, 1, w), jnp.float32)] * 6,
                *[pltpu.VMEM((4, 1, w), jnp.float32)] * 3,
                *[pltpu.VMEM((2, d, w), jnp.bfloat16)] * 3,
                pltpu.SemaphoreType.DMA((3,)),
                pltpu.SemaphoreType.DMA((1,)),
                *[pltpu.SemaphoreType.DMA((kvh,))] * 4,
            ],
            compiler_params=pltpu.CompilerParams(
                collective_id=0, has_side_effects=True, vmem_limit_bytes=40 * 2**20),
            name='ring_attention',
        )(*operands)
        out = pl.pallas_call(
            functools.partial(last_kernel, scale=d ** -0.5),
            out_shape=jax.ShapeDtypeStruct((t, kvh, gq, d), jnp.bfloat16),
            in_specs=[vmem] * 6,
            out_specs=any_spec,
            scratch_shapes=[
                pltpu.VMEM((t, gq, d), jnp.bfloat16),
                pltpu.VMEM((12 * ch, w), jnp.float32),
                pltpu.VMEM((12 * ch, w), jnp.bfloat16),
                pltpu.SemaphoreType.DMA((kvh + 3,)),
            ],
            compiler_params=pltpu.CompilerParams(vmem_limit_bytes=16 * 2**20),
            name='write_result',
        )(*states)
        return out.reshape(t, h, d)

    return jax.shard_map(local, mesh=mesh, in_specs=(spec, spec, spec), out_specs=spec, check_vma=False)
```

```python
import functools
import math

import jax
import jax.numpy as jnp
from jax import lax
from jax.experimental import pallas as pl
from jax.experimental.pallas import tpu as pltpu
from jax.sharding import PartitionSpec as P

MESH = pl.DeviceIdType.MESH
AHEAD = 3
QT = 32
NT = 3
NEG = -jnp.inf


def chunks_of(chip):
    far = 3 - chip
    early_low = [(0, j) for j in range(chip + 1) if j != far]
    late_low = [(0, far)] if far <= chip else []
    early_high = early_low + [(0, j) for j in range(chip + 1, 4) if j != far]
    early_high += [(1, j) for j in range(3, chip - 1, -1) if j != far]
    late_high = [(0, far)] + ([(1, far)] if far >= chip else [])
    return early_high, early_low, late_high, late_low


def kernel(q_hbm, k_hbm, v_hbm, o_ref, q_last, kv_last, mk, lk, acck, q_s, raw, f32s, kv, vte, vtl, *rest,
           scale):
    s_s, p_s, m_s, al_s, be_s, l_s, fin_s = (rest[3 * i:3 * i + 3] for i in range(7))
    load_sem, send_sem, xy_sem, dg_sem, se_sem, sl_sem = rest[21:]
    G, T, GQ, D = q_s.shape
    CH = T // 2
    C2 = 2 * CH
    W = QT * GQ
    cb = lax.axis_index('batch')
    cy = lax.axis_index('cy')
    cx = lax.axis_index('cx')
    ox = lax.rem(cx + 2, 4)
    sx = cx + 1 - 2 * lax.rem(cx, 2)
    oy = 1 - cy
    x_dev = (cb, cy, ox)
    y_dev = (cb, oy, cx)
    s_dev = (cb, cy, sx)
    me = cy * 4 + cx
    rx, ry, rd = cy * 4 + ox, oy * 4 + cx, oy * 4 + ox
    odd = lax.rem(cx, 2)
    chip_of = me // 2

    kcopy = pltpu.make_async_copy(k_hbm, raw.at[0], load_sem.at[0])
    vcopy = pltpu.make_async_copy(v_hbm, raw.at[1], load_sem.at[1])
    kcopy.start()
    vcopy.start()

    barrier = pltpu.get_barrier_semaphore()
    for dev in (x_dev, y_dev, s_dev):
        pl.semaphore_signal(barrier, inc=1, device_id=dev, device_id_type=MESH)

    for g in range(G):
        pltpu.make_async_copy(q_hbm.at[:, g], q_s.at[g], load_sem.at[2]).start()

    def take(g):
        for which in (0, 1):
            rows = f32s[which, pl.ds(g, T, stride=G), :].astype(jnp.bfloat16)
            kv[g, 2 * me, which] = rows[:CH]
            kv[g, 2 * me + 1, which] = rows[CH:]

    for which, copy in ((0, kcopy), (1, vcopy)):
        copy.wait()
        f32s[which] = raw[which].astype(jnp.float32).reshape(T * G, D)
    for g in range(AHEAD):
        take(g)

    pl.semaphore_wait(barrier, 3)

    def piece(g, r, full):
        return kv.at[g, pl.ds(2 * r, 2)] if full else kv.at[g, 2 * r]

    def send(g, ref, recv_sem, dev):
        pltpu.make_async_remote_copy(
            src_ref=ref, dst_ref=ref, send_sem=send_sem.at[0], recv_sem=recv_sem.at[g],
            device_id=dev, device_id_type=MESH).start()

    def arrived(g, count, recv_sem):
        ref = kv.at[g, 0:count]
        pltpu.make_async_remote_copy(
            src_ref=ref, dst_ref=ref, send_sem=send_sem.at[0], recv_sem=recv_sem.at[g],
            device_id=x_dev, device_id_type=MESH).wait_recv()

    c2 = scale * math.log2(math.e)
    sub = lax.broadcasted_iota(jnp.int32, (8, W), 0)
    base = sub - lax.broadcasted_iota(jnp.int32, (8, W), 1) // GQ

    def keys(g, chunk_list, which):
        parts = [kv[g, 4 * j + half + 2 * core, which] for half, j in chunk_list for core in (0, 1)]
        return jnp.concatenate(parts, axis=0)

    def pipeline(chip):
        xc, yc, far = chip ^ 1, chip ^ 2, chip ^ 3
        own_x, own_y = True, True
        got_x, got_y, got_far = True, True, True
        cross_high = True
        n_xy = 2 + got_x + got_y
        n_far = 1 + got_far
        n_sent = (2 + own_x + own_y) + 2 + (1 + cross_high) + (2 + got_x + got_y) + n_far

        def start_own(g):
            send(g, piece(g, me, own_x), xy_sem, x_dev)
            send(g, piece(g, me, own_y), xy_sem, y_dev)
            send(g, piece(g, me, True), se_sem, s_dev)

        def forward(g):
            arrived(g, n_xy, xy_sem)
            send(g, kv.at[g, 2 * rx], dg_sem, y_dev)
            if cross_high:
                send(g, kv.at[g, 2 * ry + 1], dg_sem, x_dev)
            send(g, piece(g, rx, got_x), se_sem, s_dev)
            send(g, piece(g, ry, got_y), se_sem, s_dev)

        def diagonal(g):
            arrived(g, n_far, dg_sem)
            send(g, piece(g, rd, got_far), sl_sem, s_dev)

        for g in range(AHEAD):
            start_own(g)
        for g in range(AHEAD, G):
            take(g)
        pltpu.make_async_copy(q_s, q_s, load_sem.at[2]).wait()
        q_last[...] = q_s[G - 1]

        lists = chunks_of(chip)
        names = ('eh', 'el', 'lh', 'll')
        rows = {}
        at = 0
        for name, lst in zip(names, lists):
            rows[name] = (at, C2 * len(lst))
            at += C2 * len(lst)
        lst = dict(zip(names, lists))
        halves = (1, 0)

        def transposed(g, slot, names):
            for name, ref in names:
                n = rows[name][1]
                ref[slot, :, :n] = keys(g, lst[name], 1).T

        def split(u):
            return lax.div(u + NT, NT) - 1, lax.rem(u + NT, NT)

        def score(g, t, half, name, slot, masked):
            at, n = rows[name]
            qv = q_s[g, pl.ds(half * CH + t * QT, QT)].reshape(W, D)
            s = lax.dot_general(keys(g, lst[name], 0), qv, (((1,), (1,)), ((), ())),
                                preferred_element_type=jnp.float32)
            edge = n - C2 if masked else n
            top = None
            if edge:
                s_s[slot][at:at + edge] = s[:edge]
                for i in range(edge // 8):
                    si = s[8 * i:8 * i + 8]
                    top = si if top is None else jnp.maximum(top, si)
            if masked:
                thr = t * QT + CH * (odd if half == 0 else -odd)
                for i in range(C2 // 8):
                    first = 8 * i if (half == 0 or i < CH // 8) else 8 * i - C2
                    si = jnp.where(base <= thr - first, s[edge + 8 * i:edge + 8 * i + 8], NEG)
                    s_s[slot][at + edge + 8 * i:at + edge + 8 * i + 8] = si
                    top = si if top is None else jnp.maximum(top, si)
            return jnp.max(top, axis=0, keepdims=True)

        def stage_a(u, slot, early=True, late=True):
            g, t = split(u)
            par = lax.rem(g + 2, 2)
            gl = jnp.where(g < 2, G, g - 2)
            ql = jnp.maximum(g - 2, 0)
            for half in halves:
                e, l = ('eh', 'lh') if half else ('el', 'll')
                if late and lst[l]:
                    old = mk[par, half, t]
                    m = jnp.maximum(score_late(gl, ql, t, half, l, slot), old)
                    m_s[slot][2 + half] = m
                    al_s[slot][half] = jnp.exp2((old - m) * c2)
                if early:
                    m = score(g, t, half, e, slot, True)
                    m_s[slot][half] = m
                    mk[par, half, t] = m

        def score_late(gl, ql, t, half, name, slot):
            at, n = rows[name]
            qv = q_s[ql, pl.ds(half * CH + t * QT, QT)].reshape(W, D)
            s = lax.dot_general(keys(gl, lst[name], 0), qv, (((1,), (1,)), ((), ())),
                                preferred_element_type=jnp.float32)
            s_s[slot][at:at + n] = s
            top = s[:8]
            for i in range(1, n // 8):
                top = jnp.maximum(top, s[8 * i:8 * i + 8])
            return jnp.max(top, axis=0, keepdims=True)

        def weights(name, slot, m):
            at, n = rows[name]
            total = None
            for j in range(n // C2):
                sl = slice(at + j * C2, at + (j + 1) * C2)
                p = jnp.exp2((s_s[slot][sl] - m) * c2)
                for i in range(C2 // 8):
                    pi = p[8 * i:8 * i + 8]
                    total = pi if total is None else total + pi
                p_s[slot][sl] = p.astype(jnp.bfloat16)
            return jnp.sum(total, axis=0, keepdims=True)

        def stage_b(u, slot, early=True, late=True):
            g, t = split(u)
            par = lax.rem(g + 2, 2)
            for half in halves:
                e, l = ('eh', 'lh') if half else ('el', 'll')
                if late and lst[l]:
                    total = weights(l, slot, m_s[slot][2 + half])
                    l_s[slot][2 + half] = lk[par, half, t] * al_s[slot][half] + total
                    be_s[slot][half] = al_s[slot][half]
                if early:
                    total = weights(e, slot, m_s[slot][half])
                    l_s[slot][half] = total
                    lk[par, half, t] = total

        def values(name, ref, par, slot):
            at, n = rows[name]
            return lax.dot_general(ref[par, :, :n], p_s[slot][at:at + n], (((1,), (0,)), ((), ())),
                                   preferred_element_type=jnp.float32)

        def put(slot, half, acc, total):
            fin_s[slot][half] = (acc * (1.0 / total)).astype(jnp.bfloat16)

        def stage_d(u, slot, late_only=False):
            g, t = split(u)
            for half in halves:
                late = bool(lst['lh' if half else 'll'])
                if late or not late_only:
                    to = jnp.maximum(g - 2, 0) if late else jnp.maximum(g, 0)
                    o_ref[pl.ds(half * CH + t * QT, QT), to] = fin_s[slot][half].T.reshape(QT, GQ, D)

        def stage_c(u, slot, early=True, late=True):
            g, t = split(u)
            par = lax.rem(g + 2, 2)
            ge = jnp.maximum(g, 0)
            gl = jnp.maximum(g - 2, 0)
            for half in halves:
                e, l = ('eh', 'lh') if half else ('el', 'll')
                if late and lst[l]:
                    acc = acck[par, half, t] * be_s[slot][half] + values(l, vtl, lax.rem(gl, 2), slot)
                    put(slot, half, acc, l_s[slot][2 + half])
                if early:
                    acc = values(e, vte, lax.rem(ge, 2), slot)
                    if lst[l]:
                        acck[par, half, t] = acc
                    else:
                        put(slot, half, acc, l_s[slot][half])

        def service(g):
            arrived(g, 2 + n_xy, se_sem)

            @pl.when(g > 1)
            def _():
                arrived(g - 2, n_far, sl_sem)
                transposed(g - 2, lax.rem(g, 2), (('lh', vtl),))
            transposed(g, lax.rem(g, 2), (('eh', vte),))

        n = NT * G
        forward(0)
        start_own(AHEAD)

        def body(pair, carry):
            for odd_i in (0, 1):
                i = 2 * pair + odd_i

                @pl.when(lax.rem(i, NT) == 0)
                def _(i=i):
                    service(lax.div(i, NT))

                @pl.when(jnp.logical_and(lax.rem(i, NT) == 1, i < n - NT))
                def _(i=i):
                    forward(lax.div(i, NT) + 1)

                @pl.when(jnp.logical_and(lax.rem(i, NT) == 2, i < n - NT - NT * AHEAD))
                def _(i=i):
                    start_own(lax.div(i, NT) + 1 + AHEAD)

                @pl.when(jnp.logical_and(lax.rem(i, NT) == 2, i >= NT))
                def _(i=i):
                    diagonal(lax.div(i, NT) - 1)

                stage_a(i, odd_i)
                stage_b(i - 1, 1 - odd_i)
                stage_c(i - 1, 1 - odd_i)
                stage_d(i - 2, odd_i)
            return carry

        lax.fori_loop(0, n // 2, body, 0)
        diagonal(G - 1)
        stage_b(n - 1, 1 - n % 2)
        stage_c(n - 1, 1 - n % 2)
        stage_d(n - 2, n % 2)
        stage_d(n - 1, 1 - n % 2)

        arrived(G - 2, n_far, sl_sem)
        transposed(G - 2, G % 2, (('lh', vtl),))
        for t in range(NT):
            stage_a(n + t, t, early=False)
        for t in range(NT):
            stage_b(n + t, t, early=False)
        for t in range(NT):
            stage_c(n + t, t, early=False)
            stage_d(n + t, t, late_only=True)
        arrived(G - 1, n_far, sl_sem)
        for i, (half, j) in enumerate(lst['lh']):
            for core in (0, 1):
                kv_last[2 * i + core] = kv[G - 1, 4 * j + half + 2 * core]

        ref = kv.at[0:G, 0:n_sent]
        pltpu.make_async_remote_copy(
            src_ref=ref, dst_ref=ref, send_sem=send_sem.at[0], recv_sem=xy_sem.at[0],
            device_id=x_dev, device_id_type=MESH).wait_send()

    for chip in range(4):
        @pl.when(chip_of == chip)
        def _(chip=chip):
            pipeline(chip)


def last_kernel(o_part, q_last, kv_last, mk, lk, acck, o_hbm, out_s, s_s, p_s, sem, *, scale):
    T, G, GQ, D = o_part.shape
    CH = T // 2
    W = QT * GQ
    chip_of = lax.axis_index('cy') * 2 + lax.axis_index('cx') // 2
    step = T
    copies = [pltpu.make_async_copy(o_part.at[pl.ds(i * step, step), pl.ds(0, G - 1)],
                                    o_hbm.at[pl.ds(i * step, step), pl.ds(0, G - 1)], sem.at[i]) for i in range(1)]
    for c in copies:
        c.start()
    c2 = scale * math.log2(math.e)
    last = (G - 1) % 2

    def merge(chip):
        late_high, late_low = chunks_of(chip)[2:]
        tiles = [(1, t, len(late_high)) for t in range(NT)]
        tiles += [(0, t, len(late_low)) for t in range(NT) if late_low]
        ends = []
        if not late_low:
            ends.append(pltpu.make_async_copy(o_part.at[pl.ds(0, CH), G - 1], o_hbm.at[pl.ds(0, CH), G - 1], sem.at[1]))
            ends[0].start()
        n_pieces = 2 * len(late_high)
        keys = kv_last[0:n_pieces, 0].reshape(n_pieces * CH, D)
        vals = kv_last[0:n_pieces, 1].reshape(n_pieces * CH, D).T
        slabs = lambda x: [x[8 * i:8 * i + 8] for i in range(x.shape[0] // 8)]
        tops, sums, at = [], [], 0
        for half, t, count in tiles:
            n = 2 * CH * count
            rows = slice(half * CH + t * QT, half * CH + (t + 1) * QT)
            s = lax.dot_general(keys[:n], q_last[rows].reshape(W, D), (((1,), (1,)), ((), ())),
                                preferred_element_type=jnp.float32)
            s_s[at:at + n] = s
            top = functools.reduce(jnp.maximum, slabs(s))
            tops.append(jnp.maximum(jnp.max(top, axis=0, keepdims=True), mk[last, half, t]))
            at += n
        at = 0
        for (half, t, count), m in zip(tiles, tops):
            n = 2 * CH * count
            total = None
            for j in range(count):
                sl = slice(at + j * 2 * CH, at + (j + 1) * 2 * CH)
                p = jnp.exp2((s_s[sl] - m) * c2)
                part = functools.reduce(jnp.add, slabs(p))
                total = part if total is None else total + part
                p_s[sl] = p.astype(jnp.bfloat16)
            sums.append(jnp.sum(total, axis=0, keepdims=True))
            at += n
        at = 0
        for (half, t, count), m, total in zip(tiles, tops, sums):
            n = 2 * CH * count
            rows = slice(half * CH + t * QT, half * CH + (t + 1) * QT)
            alpha = jnp.exp2((mk[last, half, t] - m) * c2)
            inv = 1.0 / (lk[last, half, t] * alpha + total)
            acc = acck[last, half, t] * (alpha * inv) + lax.dot_general(
                vals[:, :n], p_s[at:at + n], (((1,), (0,)), ((), ())), preferred_element_type=jnp.float32) * inv
            out_s[rows] = acc.astype(jnp.bfloat16).T.reshape(QT, GQ, D)
            at += n
        for half in ((1, 0) if late_low else (1,)):
            ends.append(pltpu.make_async_copy(
                out_s.at[pl.ds(half * CH, CH)], o_hbm.at[pl.ds(half * CH, CH), G - 1], sem.at[2 + half]))
            ends[-1].start()
        for c in ends:
            c.wait()

    for chip in range(4):
        @pl.when(chip_of == chip)
        def _(chip=chip):
            merge(chip)

    for c in copies:
        c.wait()


def solution(mesh):
    spec = P(('batch', 'cy', 'cx'), None, None)

    def local(q, k, v):
        t, h, d = q.shape
        kvh = k.shape[1]
        gq = h // kvh
        ch = t // 2
        ndev = mesh.shape['cy'] * mesh.shape['cx']
        w = QT * gq
        rows = 9 * 2 * ch
        any_spec = pl.BlockSpec(memory_space=pltpu.HBM)
        operands = [pltpu.with_memory_space_constraint(x, pltpu.HBM) for x in (q.reshape(t, kvh, gq, d), k, v)]
        states = [
            jax.ShapeDtypeStruct((t, kvh, gq, d), jnp.bfloat16),
            jax.ShapeDtypeStruct((t, gq, d), jnp.bfloat16),
            jax.ShapeDtypeStruct((4, 2, ch, d), jnp.bfloat16),
            jax.ShapeDtypeStruct((2, 2, NT, 1, w), jnp.float32),
            jax.ShapeDtypeStruct((2, 2, NT, 1, w), jnp.float32),
            jax.ShapeDtypeStruct((2, 2, NT, d, w), jnp.float32),
        ]
        vmem = pl.BlockSpec(memory_space=pltpu.VMEM)
        states = pl.pallas_call(
            functools.partial(kernel, scale=d ** -0.5),
            out_shape=states,
            in_specs=[any_spec] * 3,
            out_specs=[vmem] * 6,
            scratch_shapes=[
                pltpu.VMEM((kvh, t, gq, d), jnp.bfloat16),
                pltpu.VMEM((2, t, kvh, d), jnp.bfloat16),
                pltpu.VMEM((2, t * kvh, d), jnp.float32),
                pltpu.VMEM((kvh + 1, 2 * ndev, 2, ch, d), jnp.bfloat16),
                pltpu.VMEM((2, d, 12 * ch), jnp.bfloat16),
                pltpu.VMEM((2, d, 4 * ch), jnp.bfloat16),
                *[pltpu.VMEM((rows, w), jnp.float32)] * 3,
                *[pltpu.VMEM((rows, w), jnp.bfloat16)] * 3,
                *[pltpu.VMEM((4, 1, w), jnp.float32)] * 3,
                *[pltpu.VMEM((2, 1, w), jnp.float32)] * 6,
                *[pltpu.VMEM((4, 1, w), jnp.float32)] * 3,
                *[pltpu.VMEM((2, d, w), jnp.bfloat16)] * 3,
                pltpu.SemaphoreType.DMA((3,)),
                pltpu.SemaphoreType.DMA((1,)),
                *[pltpu.SemaphoreType.DMA((kvh,))] * 4,
            ],
            compiler_params=pltpu.CompilerParams(
                collective_id=0, has_side_effects=True, vmem_limit_bytes=40 * 2**20),
            name='ring_attention',
        )(*operands)
        out = pl.pallas_call(
            functools.partial(last_kernel, scale=d ** -0.5),
            out_shape=jax.ShapeDtypeStruct((t, kvh, gq, d), jnp.bfloat16),
            in_specs=[vmem] * 6,
            out_specs=any_spec,
            scratch_shapes=[
                pltpu.VMEM((t, gq, d), jnp.bfloat16),
                pltpu.VMEM((12 * ch, w), jnp.float32),
                pltpu.VMEM((12 * ch, w), jnp.bfloat16),
                pltpu.SemaphoreType.DMA((4,)),
            ],
            compiler_params=pltpu.CompilerParams(vmem_limit_bytes=16 * 2**20),
            name='write_result',
        )(*states)
        return out.reshape(t, h, d)

    return jax.shard_map(local, mesh=mesh, in_specs=(spec, spec, spec), out_specs=spec, check_vma=False)
```
